128 devices in a mesh: atom: 32 (over y, z, core), aux: 4 (over x).
Axes of the slice: x: 4, y: 4, z: 4, core: 2. Of those that a mesh axis runs over, the one named last changes fastest.
Arguments:
- pao_blocks: bfloat16 [64, 24, 15360], P('atom', None, 'aux'), may hold values from -0.048339844 to 0.048339844
- cabs_blocks: bfloat16 [64, 48, 15360], P('atom', None, 'aux'), may hold values from -0.3046875 to 0.3046875
- cabs_weight: bfloat16 [64, 48], P('atom'), may hold values from 0.25 to 4
- pair_blocks: int32 [2048, 4], P('atom'), may hold values from 0 to 63, as said below
- pao_size: int32 [2048], P('atom'), may hold values from 24 to 96
- cabs_size: int32 [2048], P('atom'), may hold values from 48 to 192
Outputs:
- v_pairs: float32 [2048, 96, 96], P('atom', 'aux')
The draws below stay inside these ranges and needn't reach their ends.
Inputs may be any that keep to these rules, and one draw needn't show every extreme that they name: `pair_blocks`: each row names 4 different atom blocks; atom block b belongs to owner b // 2, and the 64 rows of one index of atom name at most one block of each owner.
All inputs are finite; a program needn't handle non-finite values.
Results may differ from the reference program's by a relative error of at most 0.0003.
Values may be sent and summed in bfloat16 or wider, within the bound.
A program may use at most 128 MiB of HBM per device.

```python
import math
import jax
import jax.numpy as jnp
from jax import lax

AUX = 15360
RB = 24
RBC = 48
BLK_DEV = 2
DOM_BLOCKS = 4
PAIR_DEV = 64
NBLK = 64
PAIRS = 2048
DA = 96
DC = 192


def draw_pair_blocks(key, part):
    owners = NBLK // BLK_DEV
    devices = PAIRS // PAIR_DEV
    subkeys = jax.random.split(key, 5)
    ordering = jax.vmap(lambda subkey: jax.random.permutation(subkey, owners))(jax.random.split(subkeys[0], devices))
    used_count = jax.random.randint(subkeys[1], (devices,), DOM_BLOCKS, owners + 1)
    fullest = jax.random.randint(subkeys[2], (), 0, devices)
    used_count = jnp.where(jnp.arange(devices) == fullest, owners, used_count)
    local_pick = jax.random.randint(subkeys[3], (devices, owners), 0, BLK_DEV)
    scores = jax.vmap(lambda subkey: jax.random.permutation(subkey, owners))(jax.random.split(subkeys[4], devices * PAIR_DEV))
    scores = scores.reshape(devices, PAIR_DEV, owners)
    position = jnp.arange(owners)
    scores = scores + owners * (position[None, None, :] >= used_count[:, None, None]).astype(jnp.int32)
    picked = jnp.argsort(scores, axis=-1, stable=True)[:, :, :DOM_BLOCKS]
    owner_ids = jnp.take_along_axis(jnp.broadcast_to(ordering[:, None, :], scores.shape), picked, axis=-1)
    chosen_local = jnp.take_along_axis(jnp.broadcast_to(local_pick[:, None, :], scores.shape), owner_ids, axis=-1)
    blocks_out = owner_ids * BLK_DEV + chosen_local
    return blocks_out.reshape(PAIRS, DOM_BLOCKS).astype(jnp.int32)


def with_ends(result, key, smallest, largest):
    longest = result.shape.index(max(result.shape))
    spots = []
    for shift in (0, 1):
        where = [jax.random.randint(jax.random.fold_in(key, axis), (), 0, length) for axis, length in enumerate(result.shape)]
        where[longest] = (where[longest] + shift) % result.shape[longest]
        spots.append(tuple(where))
    return result.at[spots[0]].set(smallest).at[spots[1]].set(largest)


def block_scale(key, extent, cuts, least, high):
    level = 1.0
    for axis_at, blocks in cuts:
        steps = jax.random.uniform(jax.random.fold_in(jax.random.fold_in(key, 6), axis_at), (blocks,), jnp.float32, least / len(cuts), high / len(cuts))
        level = level * jnp.repeat(jnp.exp(steps), extent[axis_at] // blocks).reshape((-1,) + (1,) * (len(extent) - 1 - axis_at))
    return level


def noise(own_key, shape, spread, most, shards=(), kind=jnp.bfloat16):
    values = spread * jax.random.normal(own_key, shape, jnp.float32)
    if shards:
        values = values * block_scale(own_key, shape, shards, -0.22, 0.18)
    return jnp.clip(values, -most, most).astype(kind)


def setup_inputs(seed: int = 0) -> dict:
    splits = jax.random.split(jax.random.key(seed), 7)
    return {
        "pao_blocks": noise(splits[0], (NBLK, RB, AUX), (AUX ** -0.5), 0.048339844, ((0, 32), (2, 4))),
        "cabs_blocks": noise(splits[1], (NBLK, RBC, AUX), ((0.5 / DC) ** 0.5), 0.3046875, ((0, 32), (2, 4))),
        "cabs_weight": jnp.clip(jnp.exp(math.log(4.0) - 2.7725887 * jax.random.uniform(splits[2], (NBLK, RBC), jnp.float32) ** block_scale(splits[2], (NBLK, RBC), ((0, 32),), -0.2, 0.2)), 0.25, 4.0).astype(jnp.bfloat16),
        "pair_blocks": draw_pair_blocks(jax.random.fold_in(splits[6], 71), 0),
        "pao_size": with_ends(jax.random.randint(splits[4], (PAIRS,), RB, DA + 1), jax.random.fold_in(splits[4], 1), RB, DA).astype(jnp.int32),
        "cabs_size": with_ends(jax.random.randint(splits[5], (PAIRS,), RBC, DC + 1), jax.random.fold_in(splits[5], 1), RBC, DC).astype(jnp.int32),
    }


def reference(pao_blocks, cabs_blocks, cabs_weight, pair_blocks, pao_size, cabs_size):
    flat_pao = pao_blocks.reshape(NBLK * RB, AUX)
    flat_cabs = cabs_blocks.reshape(NBLK * RBC, AUX)
    gram_pao = jnp.dot(flat_pao, flat_pao.T, preferred_element_type=jnp.float32)
    gram_cross = jnp.dot(flat_pao, flat_cabs.T, preferred_element_type=jnp.float32)
    index_pao = (pair_blocks[:, :, None] * RB + jnp.arange(RB, dtype=jnp.int32)[None, None, :]).reshape(PAIRS, DA).astype(jnp.int32)
    index_cabs = (pair_blocks[:, :, None] * RBC + jnp.arange(RBC, dtype=jnp.int32)[None, None, :]).reshape(PAIRS, DC).astype(jnp.int32)
    margin = gram_pao[index_pao[:, :, None], index_pao[:, None, :]]
    coupling = gram_cross[index_pao[:, :, None], index_cabs[:, None, :]]
    keep_pao = (jnp.arange(DA, dtype=jnp.int32)[None, :] < pao_size[:, None]).astype(jnp.float32)
    keep_cabs = (jnp.arange(DC, dtype=jnp.int32)[None, :] < cabs_size[:, None]).astype(jnp.float32)
    margin = margin * keep_pao[:, :, None] * keep_pao[:, None, :]
    coupling = coupling * keep_pao[:, :, None] * keep_cabs[:, None, :]
    scales = jnp.take(cabs_weight, pair_blocks.reshape(-1), axis=0).reshape(PAIRS, DC).astype(jnp.float32)
    return margin - jnp.einsum("pix,pjx->pij", coupling * scales[:, None, :], coupling, precision=lax.Precision.HIGHEST)
```

```python
import jax
import jax.numpy as jnp
from jax import lax
from jax.experimental import pallas as pl
from jax.experimental.pallas import tpu as pltpu
from jax.sharding import PartitionSpec as P

TILES = 54


def pair_kernel(blk, gram, scale, out):
    x = lax.axis_index("aux")
    lane = lax.broadcasted_iota(jnp.int32, (8, 128), 1)

    def one_pair(p):
        picks = [blk[p * 4 + l] for l in range(4)]
        acc = None
        for l in range(4):
            off = picks[l] * 24
            lt = off // 128
            rem = off - lt * 128
            nxt = jnp.minimum(lt + 1, 11)
            lm = lt - 3 * x
            mine = jnp.logical_and(lm >= 0, lm < 3)
            lm0 = jnp.clip(lm, 0, 2)
            lm1 = jnp.clip(lm + 1, 0, 2)
            first, second = [], []
            for k in range(4):
                base = (picks[k] // 2) * TILES
                par = picks[k] % 2
                for t in range(3):
                    row = base + (par * 3 + t) * 3
                    first.append(gram[row + lm0])
                    second.append(gram[row + lm1])
            for k in range(4):
                base = (picks[k] // 2) * TILES + 18
                par = picks[k] % 2
                for ct in (par, 2):
                    first.append(gram[base + ct * 12 + lt])
                    second.append(gram[base + ct * 12 + nxt])
            a = jnp.concatenate(first, axis=0)
            b = jnp.concatenate(second, axis=0)
            lanes = lax.broadcasted_iota(jnp.int32, a.shape, 1)
            rows = lax.broadcasted_iota(jnp.int32, a.shape, 0)
            both = jnp.where(lanes >= rem, a, b)
            keep = jnp.logical_or(rows >= 96, mine)
            both = jnp.where(keep, both, 0.0)
            turned = pltpu.roll(both, lax.rem(24 * l - rem + 128, 128), 1)
            if acc is None:
                acc = jnp.where(lanes < 24, turned, 0.0)
            else:
                here = jnp.logical_and(lanes >= 24 * l, lanes < 24 * l + 24)
                acc = jnp.where(here, turned, acc)
        margin, c = acc[:96], acc[96:]
        cs = c * scale[p]
        c_hi = c.astype(jnp.bfloat16)
        c_lo = (c - c_hi.astype(jnp.float32)).astype(jnp.bfloat16)
        s_hi = cs.astype(jnp.bfloat16)
        s_lo = (cs - s_hi.astype(jnp.float32)).astype(jnp.bfloat16)
        left = jnp.concatenate([s_hi, s_lo, s_hi], axis=0)
        right = jnp.concatenate([c_hi, c_hi, c_lo], axis=0)
        prod = lax.dot_general(
            left, right, (((0,), (0,)), ((), ())), preferred_element_type=jnp.float32
        )
        return margin - prod[:96]

    @pl.loop(0, 16)
    def _(g):
        v = [one_pair(g * 4 + q) for q in range(4)]
        lanes = lax.broadcasted_iota(jnp.int32, (96, 128), 1)
        r1 = pltpu.roll(v[1], 96, 1)
        r2 = pltpu.roll(v[2], 64, 1)
        r3 = pltpu.roll(v[3], 32, 1)
        out[g, :, 0:128] = jnp.where(lanes < 96, v[0], r1)
        out[g, :, 128:256] = jnp.where(lanes < 64, r1, r2)
        out[g, :, 256:384] = jnp.where(lanes < 32, r2, r3)


def pair_parts(blk, gram, scale):
    return pl.pallas_call(
        pair_kernel,
        out_shape=jax.ShapeDtypeStruct((16, 96, 384), jnp.float32),
        in_specs=[
            pl.BlockSpec(memory_space=pltpu.SMEM),
            pl.BlockSpec(memory_space=pltpu.VMEM),
            pl.BlockSpec(memory_space=pltpu.VMEM),
        ],
        out_specs=pl.BlockSpec(memory_space=pltpu.VMEM),
        compiler_params=pltpu.CompilerParams(vmem_limit_bytes=60 * 1024 * 1024),
    )(blk, gram, scale)


def by_class(rows):
    parts = rows.reshape(2, 4, 12, rows.shape[-1])
    head = parts[:, :, :8].transpose(1, 0, 2, 3).reshape(4, 16, -1)
    tail = parts[:, :, 8:].transpose(1, 0, 2, 3).reshape(4, 8, -1)
    return jnp.concatenate([head, tail], axis=1).reshape(96, -1)


def tiled(a):
    r, c = a.shape
    return a.reshape(r // 8, 8, c // 128, 128).transpose(0, 2, 1, 3).reshape(-1, 8, 128)


def shards(pao_blocks, cabs_blocks, cabs_weight, pair_blocks, pao_size, cabs_size):
    x = lax.axis_index("aux")
    every = lax.all_gather(pao_blocks.reshape(48, -1), "atom", axis=0, tiled=True)
    own = jnp.concatenate([pao_blocks.reshape(48, -1), by_class(cabs_blocks)], axis=0)
    gram = lax.dot_general(
        own, every, (((1,), (1,)), ((), ())), preferred_element_type=jnp.float32
    )
    margin = lax.psum_scatter(gram[:48], "aux", scatter_dimension=1, tiled=True)
    coupling = lax.psum_scatter(gram[48:], "aux", scatter_dimension=0, tiled=True)
    held = jnp.concatenate([tiled(margin), tiled(coupling)], axis=0)
    grams = lax.all_gather(held, "atom", axis=0, tiled=True)

    weights = lax.all_gather(cabs_weight, "atom", axis=0, tiled=True)
    mine = lax.dynamic_slice_in_dim(weights, 12 * x, 12, axis=1).astype(jnp.float32)
    picked = jnp.take(mine, pair_blocks.reshape(-1), axis=0).reshape(64, 4, 12)
    at = (
        48 * jnp.arange(4, dtype=jnp.int32)[None, :, None]
        + 12 * x
        + jnp.arange(12, dtype=jnp.int32)[None, None, :]
    )
    picked = jnp.where(at < cabs_size[:, None, None], picked, 0.0)
    odd = (pair_blocks % 2 == 1)[:, :, None]
    tail = picked[:, :, 8:]
    zero = jnp.zeros_like(tail)
    scale = jnp.concatenate(
        [picked[:, :, :8], jnp.where(odd, zero, tail), jnp.where(odd, tail, zero)], axis=2
    ).reshape(64, 64)
    scale = jnp.broadcast_to(scale[:, :, None], (64, 64, 128))

    parts = pair_parts(pair_blocks.reshape(-1), grams, scale)
    rows = lax.psum_scatter(parts, "aux", scatter_dimension=1, tiled=True)
    rows = rows.reshape(16, 24, 4, 96).transpose(0, 2, 1, 3).reshape(64, 24, 96)
    size = pao_size[:, None, None]
    keep_row = (24 * x + jnp.arange(24, dtype=jnp.int32))[None, :, None] < size
    keep_col = jnp.arange(96, dtype=jnp.int32)[None, None, :] < size
    return jnp.where(jnp.logical_and(keep_row, keep_col), rows, 0.0)


def solution(mesh):
    placed = (
        P("atom", None, "aux"),
        P("atom", None, "aux"),
        P("atom", None),
        P("atom", None),
        P("atom"),
        P("atom"),
    )
    return jax.shard_map(
        shards, mesh=mesh, in_specs=placed, out_specs=P("atom", "aux", None), check_vma=False
    )
```

```python
import functools

import jax
import jax.numpy as jnp
from jax import lax
from jax.experimental import pallas as pl
from jax.experimental.pallas import tpu as pltpu
from jax.sharding import PartitionSpec as P

MESH = pl.DeviceIdType.MESH

TILES = 54
HELD = 55


class Place:
    def __init__(self):
        self.me = lax.axis_index("atom")
        self.x = lax.axis_index("aux")
        self.core = lax.rem(self.me, 2)
        self.z = lax.rem(self.me // 2, 4)
        self.y = self.me // 8

    def atom(self, y=0, z=0, flip=False):
        core = 1 - self.core if flip else self.core
        return (lax.rem(self.y + y + 4, 4) * 4 + lax.rem(self.z + z + 4, 4)) * 2 + core

    def along(self, axis, step):
        at = self.atom(**{axis: step})
        return (at, self.x)

    def partner(self):
        return (self.atom(flip=True), self.x)

    def beside(self, step):
        return (self.me, lax.rem(self.x + step + 4, 4))


def greet(devices):
    barrier = pltpu.get_barrier_semaphore()
    for device in devices:
        pl.semaphore_signal(barrier, inc=1, device_id=device, device_id_type=MESH)
    pl.semaphore_wait(barrier, len(devices))


class Wires:
    def __init__(self, send_sem, recv_sem):
        self.send_sem, self.recv_sem, self.sent = send_sem, recv_sem, []

    def copy(self, src, dst, at, device):
        return pltpu.make_async_remote_copy(
            src_ref=src,
            dst_ref=dst,
            send_sem=self.send_sem.at[at],
            recv_sem=self.recv_sem.at[at],
            device_id=device,
            device_id_type=MESH,
        )

    def send(self, src, dst, at, device):
        copy = self.copy(src, dst, at, device)
        copy.start()
        self.sent.append(copy)

    def wait(self, view, at, device):
        self.copy(view, view, at, device).wait_recv()

    def drain(self):
        for copy in self.sent:
            copy.wait_send()
        self.sent = []


OFFSETS = (0, -1, 1, 2)
PER_HALF = 36


def gather_plane(place, wires, own, full, sub):
    axes = (("z", "y"), ("y", "z"))

    def origin(h, k, m, flip=False):
        first, second = axes[h]
        return place.atom(flip=flip, **{first: OFFSETS[k], second: OFFSETS[m]})

    def one(h, k, m):
        return full(h, origin(h, k, m))

    def to(h, order, step):
        return place.along(axes[h][order], step)

    def base(h):
        return h * PER_HALF

    def across(h, k, m):
        src = own(h) if (k, m) == (0, 0) else one(h, k, m)
        wires.send(src, one(h, k, m), base(h) + 20 + 4 * k + m, place.partner())

    def spread(h, k):
        src = own(h) if k == 0 else one(h, k, 0)
        dst = one(h, k, 0)
        wires.send(src, dst, base(h) + 4 + 4 * k, to(h, 1, 1))
        wires.send(src, dst, base(h) + 5 + 4 * k, to(h, 1, -1))

    halves = (0, 1)
    for h in halves:
        wires.send(own(h), one(h, 0, 0), base(h), to(h, 0, 1))
        wires.send(own(h), one(h, 0, 0), base(h) + 1, to(h, 0, -1))
    for h in halves:
        spread(h, 0)
        across(h, 0, 0)
    for h in halves:
        for s, step in ((0, 1), (1, -1)):
            k = s + 1
            wires.wait(one(h, k, 0), base(h) + s, to(h, 0, step))
            piece = sub(h, origin(h, k, 0), s)
            wires.send(piece, piece, base(h) + 2 + s, to(h, 0, step))
    for h in halves:
        for k in (1, 2):
            spread(h, k)
            across(h, k, 0)

    def forward(h, k):
        for s, step in ((0, 1), (1, -1)):
            m = s + 1
            wires.wait(one(h, k, m), base(h) + 4 + 4 * k + s, to(h, 1, step))
            piece = sub(h, origin(h, k, m), s)
            wires.send(piece, piece, base(h) + 6 + 4 * k + s, to(h, 1, step))
            across(h, k, m)

    for h in halves:
        forward(h, 0)
    for h in halves:
        for s, step in ((0, 1), (1, -1)):
            wires.wait(sub(h, origin(h, 3, 0), s), base(h) + 2 + s, to(h, 0, step))
        spread(h, 3)
        across(h, 3, 0)
    for k in (1, 2, 3):
        for h in halves:
            forward(h, k)
    for k in range(4):
        for h in halves:
            for s, step in ((0, 1), (1, -1)):
                wires.wait(
                    sub(h, origin(h, k, 3), s), base(h) + 6 + 4 * k + s, to(h, 1, step)
                )
            across(h, k, 3)
    for k in range(4):
        for m in range(4):
            for h in halves:
                view = full(h, origin(h, k, m, flip=True))
                wires.wait(view, base(h) + 20 + 4 * k + m, place.partner())


def gram_kernel(
    pao, own, weight, held, every, part, near, final,
    send_a, recv_a, send_b, recv_b, send_c, recv_c, local,
):
    place = Place()
    x = place.x
    greet(
        [place.along(a, s) for a in ("y", "z") for s in (1, -1)]
        + [place.partner(), place.beside(1), place.beside(-1)]
    )
    keep = [
        pltpu.make_async_copy(
            pao.at[:, pl.ds(1920 * h, 1920)], every.at[h, place.me], local.at[h]
        )
        for h in range(2)
    ]
    for copy in keep:
        copy.start()
    wires = Wires(send_a, recv_a)
    cuts = ((0, 1024), (1024, 896))
    gather_plane(
        place,
        wires,
        lambda h: pao.at[:, pl.ds(1920 * h, 1920)],
        lambda h, atom: every.at[h, atom],
        lambda h, atom, s: every.at[h, atom, :, pl.ds(*cuts[s])],
    )
    for copy in keep:
        copy.wait()

    nt = (((1,), (1,)), ((), ()))

    @pl.loop(0, 4)
    def _(line):
        g = None
        for h in range(2):
            rows = every[h, pl.ds(line * 8, 8)].reshape(384, 1920)
            d = lax.dot_general(
                own[:, 1920 * h : 1920 * (h + 1)], rows, nt,
                preferred_element_type=jnp.float32,
            )
            g = d if g is None else g + d
        for r in range(6):
            for c in range(3):
                part[line, r * 3 + c] = g[8 * r : 8 * r + 8, 128 * c : 128 * c + 128]
        for k in range(4):
            for r in range(3):
                for c in range(3):
                    top = 48 + 24 * k + 8 * r
                    part[k, 18 + r * 12 + line * 3 + c] = g[
                        top : top + 8, 128 * c : 128 * c + 128
                    ]

    def klass(step):
        return lax.rem(x + step + 4, 4)

    ring = Wires(send_b, recv_b)
    a, b = pl.ds(0, 27), pl.ds(27, 27)
    left, right = place.beside(-1), place.beside(1)
    ring.send(part.at[klass(2), a], near.at[0], 0, left)
    ring.send(part.at[klass(2), b], near.at[1], 1, right)
    ring.send(part.at[klass(-1), b], final.at[0, b], 2, left)
    ring.send(part.at[klass(1), a], final.at[1, a], 3, right)
    ring.wait(near.at[0], 0, left)
    part[klass(-1), a] = part[klass(-1), a] + near[0]
    ring.send(part.at[klass(-1), a], final.at[0, a], 4, left)
    ring.wait(near.at[1], 1, right)
    part[klass(1), b] = part[klass(1), b] + near[1]
    ring.send(part.at[klass(1), b], final.at[1, b], 5, right)
    ring.wait(final.at[0, b], 2, left)
    ring.wait(final.at[1, a], 3, right)
    ring.wait(final.at[0, a], 4, left)
    ring.wait(final.at[1, b], 5, right)
    held[place.me, pl.ds(0, TILES)] = part[x] + (final[0] + final[1])
    held[place.me, TILES] = weight[...]

    out = Wires(send_c, recv_c)
    span = ((0, 28), (28, 27))
    pieces = (((0, 14), (14, 14)), ((28, 14), (42, 13)))
    gather_plane(
        place,
        out,
        lambda h: held.at[place.me, pl.ds(*span[h])],
        lambda h, atom: held.at[atom, pl.ds(*span[h])],
        lambda h, atom, s: held.at[atom, pl.ds(*pieces[h][s])],
    )
    wires.drain()
    ring.drain()
    out.drain()


def grams_of(pao, own, weight):
    dma = pltpu.SemaphoreType.DMA
    vmem = pl.BlockSpec(memory_space=pltpu.VMEM)
    return pl.pallas_call(
        gram_kernel,
        out_shape=jax.ShapeDtypeStruct((32, HELD, 8, 128), jnp.float32),
        in_specs=[vmem, vmem, vmem],
        out_specs=vmem,
        scratch_shapes=[
            pltpu.VMEM((2, 32, 48, 1920), jnp.bfloat16),
            pltpu.VMEM((4, TILES, 8, 128), jnp.float32),
            pltpu.VMEM((2, 27, 8, 128), jnp.float32),
            pltpu.VMEM((2, TILES, 8, 128), jnp.float32),
            dma((2 * PER_HALF,)),
            dma((2 * PER_HALF,)),
            dma((6,)),
            dma((6,)),
            dma((2 * PER_HALF,)),
            dma((2 * PER_HALF,)),
            dma((2,)),
        ],
        compiler_params=pltpu.CompilerParams(
            collective_id=0, has_side_effects=True, vmem_limit_bytes=48 * 1024 * 1024
        ),
        name="grams",
    )(pao, own, weight)


def pair_kernel(blk, gram, scale, out):
    x = lax.axis_index("aux")
    lane = lax.broadcasted_iota(jnp.int32, (8, 128), 1)

    def one_pair(p):
        picks = [blk[p * 4 + l] for l in range(4)]
        acc = None
        for l in range(4):
            off = picks[l] * 24
            lt = off // 128
            rem = off - lt * 128
            nxt = jnp.minimum(lt + 1, 11)
            lm = lt - 3 * x
            mine = jnp.logical_and(lm >= 0, lm < 3)
            lm0 = jnp.clip(lm, 0, 2)
            lm1 = jnp.clip(lm + 1, 0, 2)
            first, second = [], []
            for k in range(4):
                base = (picks[k] // 2) * HELD
                par = picks[k] % 2
                for t in range(3):
                    row = base + (par * 3 + t) * 3
                    first.append(gram[row + lm0])
                    second.append(gram[row + lm1])
            for k in range(4):
                base = (picks[k] // 2) * HELD + 18
                par = picks[k] % 2
                for ct in (par, 2):
                    first.append(gram[base + ct * 12 + lt])
                    second.append(gram[base + ct * 12 + nxt])
            a = jnp.concatenate(first, axis=0)
            b = jnp.concatenate(second, axis=0)
            lanes = lax.broadcasted_iota(jnp.int32, a.shape, 1)
            rows = lax.broadcasted_iota(jnp.int32, a.shape, 0)
            both = jnp.where(lanes >= rem, a, b)
            keep = jnp.logical_or(rows >= 96, mine)
            both = jnp.where(keep, both, 0.0)
            turned = pltpu.roll(both, lax.rem(24 * l - rem + 128, 128), 1)
            if acc is None:
                acc = jnp.where(lanes < 24, turned, 0.0)
            else:
                here = jnp.logical_and(lanes >= 24 * l, lanes < 24 * l + 24)
                acc = jnp.where(here, turned, acc)
        margin, c = acc[:96], acc[96:]
        cs = c * scale[p]
        c_hi = c.astype(jnp.bfloat16)
        c_lo = (c - c_hi.astype(jnp.float32)).astype(jnp.bfloat16)
        s_hi = cs.astype(jnp.bfloat16)
        s_lo = (cs - s_hi.astype(jnp.float32)).astype(jnp.bfloat16)
        left = jnp.concatenate([s_hi, s_lo, s_hi], axis=0)
        right = jnp.concatenate([c_hi, c_hi, c_lo], axis=0)
        prod = lax.dot_general(
            left, right, (((0,), (0,)), ((), ())), preferred_element_type=jnp.float32
        )
        return margin - prod[:96]

    @pl.loop(0, 16)
    def _(g):
        v = [one_pair(g * 4 + q) for q in range(4)]
        lanes = lax.broadcasted_iota(jnp.int32, (96, 128), 1)
        r1 = pltpu.roll(v[1], 96, 1)
        r2 = pltpu.roll(v[2], 64, 1)
        r3 = pltpu.roll(v[3], 32, 1)
        out[g, :, 0:128] = jnp.where(lanes < 96, v[0], r1)
        out[g, :, 128:256] = jnp.where(lanes < 64, r1, r2)
        out[g, :, 256:384] = jnp.where(lanes < 32, r2, r3)


def pair_parts(blk, gram, scale):
    return pl.pallas_call(
        pair_kernel,
        out_shape=jax.ShapeDtypeStruct((16, 96, 384), jnp.float32),
        in_specs=[
            pl.BlockSpec(memory_space=pltpu.SMEM),
            pl.BlockSpec(memory_space=pltpu.VMEM),
            pl.BlockSpec(memory_space=pltpu.VMEM),
        ],
        out_specs=pl.BlockSpec(memory_space=pltpu.VMEM),
        compiler_params=pltpu.CompilerParams(vmem_limit_bytes=60 * 1024 * 1024),
    )(blk, gram, scale)


def by_class(rows):
    parts = rows.reshape(2, 4, 12, rows.shape[-1])
    head = parts[:, :, :8].transpose(1, 0, 2, 3).reshape(4, 16, -1)
    tail = parts[:, :, 8:].transpose(1, 0, 2, 3).reshape(4, 8, -1)
    return jnp.concatenate([head, tail], axis=1).reshape(96, -1)


def shards(pao_blocks, cabs_blocks, cabs_weight, pair_blocks, pao_size, cabs_size):
    x = lax.axis_index("aux")
    pao = pao_blocks.reshape(48, -1)
    own = jnp.concatenate([pao, by_class(cabs_blocks)], axis=0)
    weight = jnp.pad(cabs_weight.astype(jnp.float32), ((0, 6), (0, 80)))
    held = grams_of(pao, own, weight)
    grams = held.reshape(32 * HELD, 8, 128)
    weights = held[:, TILES, :2, :48].reshape(64, 48)
    mine = lax.dynamic_slice_in_dim(weights, 12 * x, 12, axis=1)
    picked = jnp.take(mine, pair_blocks.reshape(-1), axis=0).reshape(64, 4, 12)
    at = (
        48 * jnp.arange(4, dtype=jnp.int32)[None, :, None]
        + 12 * x
        + jnp.arange(12, dtype=jnp.int32)[None, None, :]
    )
    picked = jnp.where(at < cabs_size[:, None, None], picked, 0.0)
    odd = (pair_blocks % 2 == 1)[:, :, None]
    tail = picked[:, :, 8:]
    zero = jnp.zeros_like(tail)
    scale = jnp.concatenate(
        [picked[:, :, :8], jnp.where(odd, zero, tail), jnp.where(odd, tail, zero)], axis=2
    ).reshape(64, 64)
    scale = jnp.broadcast_to(scale[:, :, None], (64, 64, 128))

    parts = pair_parts(pair_blocks.reshape(-1), grams, scale)
    rows = lax.psum_scatter(parts, "aux", scatter_dimension=1, tiled=True)
    rows = rows.reshape(16, 24, 4, 96).transpose(0, 2, 1, 3).reshape(64, 24, 96)
    size = pao_size[:, None, None]
    keep_row = (24 * x + jnp.arange(24, dtype=jnp.int32))[None, :, None] < size
    keep_col = jnp.arange(96, dtype=jnp.int32)[None, None, :] < size
    return jnp.where(jnp.logical_and(keep_row, keep_col), rows, 0.0)


def solution(mesh):
    placed = (
        P("atom", None, "aux"),
        P("atom", None, "aux"),
        P("atom", None),
        P("atom", None),
        P("atom"),
        P("atom"),
    )
    return jax.shard_map(
        shards, mesh=mesh, in_specs=placed, out_specs=P("atom", "aux", None), check_vma=False
    )
```

```python
import jax
import jax.numpy as jnp
from jax import lax
from jax.experimental import pallas as pl
from jax.experimental.pallas import tpu as pltpu
from jax.sharding import PartitionSpec as P

MESH = pl.DeviceIdType.MESH

TILES = 54
HELD = 55


class Place:
    def __init__(self):
        self.me = lax.axis_index("atom")
        self.x = lax.axis_index("aux")
        self.core = lax.rem(self.me, 2)
        self.z = lax.rem(self.me // 2, 4)
        self.y = self.me // 8

    def atom(self, y=0, z=0, flip=False):
        core = 1 - self.core if flip else self.core
        return (lax.rem(self.y + y + 4, 4) * 4 + lax.rem(self.z + z + 4, 4)) * 2 + core

    def along(self, axis, step):
        at = self.atom(**{axis: step})
        return (at, self.x)

    def partner(self):
        return (self.atom(flip=True), self.x)

    def beside(self, step):
        return (self.me, lax.rem(self.x + step + 4, 4))


def greet(devices):
    barrier = pltpu.get_barrier_semaphore()
    for device in devices:
        pl.semaphore_signal(barrier, inc=1, device_id=device, device_id_type=MESH)
    pl.semaphore_wait(barrier, len(devices))


class Wires:
    def __init__(self, send_sem, recv_sem):
        self.send_sem, self.recv_sem, self.sent = send_sem, recv_sem, []

    def copy(self, src, dst, at, device):
        return pltpu.make_async_remote_copy(
            src_ref=src,
            dst_ref=dst,
            send_sem=self.send_sem.at[at],
            recv_sem=self.recv_sem.at[at],
            device_id=device,
            device_id_type=MESH,
        )

    def send(self, src, dst, at, device):
        copy = self.copy(src, dst, at, device)
        copy.start()
        self.sent.append(copy)

    def wait(self, view, at, device):
        self.copy(view, view, at, device).wait_recv()

    def drain(self):
        for copy in self.sent:
            copy.wait_send()
        self.sent = []


OFFSETS = (0, -1, 1, 2)
PER_HALF = 36


def gather_plane(place, wires, own, full, sub):
    axes = (("z", "y"), ("y", "z"))

    def origin(h, k, m, flip=False):
        first, second = axes[h]
        return place.atom(flip=flip, **{first: OFFSETS[k], second: OFFSETS[m]})

    def one(h, k, m):
        return full(h, origin(h, k, m))

    def to(h, order, step):
        return place.along(axes[h][order], step)

    def base(h):
        return h * PER_HALF

    def across(h, k, m):
        src = own(h) if (k, m) == (0, 0) else one(h, k, m)
        wires.send(src, one(h, k, m), base(h) + 20 + 4 * k + m, place.partner())

    def spread(h, k):
        src = own(h) if k == 0 else one(h, k, 0)
        dst = one(h, k, 0)
        wires.send(src, dst, base(h) + 4 + 4 * k, to(h, 1, 1))
        wires.send(src, dst, base(h) + 5 + 4 * k, to(h, 1, -1))

    halves = (0, 1)
    for h in halves:
        wires.send(own(h), one(h, 0, 0), base(h), to(h, 0, 1))
        wires.send(own(h), one(h, 0, 0), base(h) + 1, to(h, 0, -1))
    for h in halves:
        spread(h, 0)
        across(h, 0, 0)
    for h in halves:
        for s, step in ((0, 1), (1, -1)):
            k = s + 1
            wires.wait(one(h, k, 0), base(h) + s, to(h, 0, step))
            piece = sub(h, origin(h, k, 0), s)
            wires.send(piece, piece, base(h) + 2 + s, to(h, 0, step))
    for h in halves:
        for k in (1, 2):
            spread(h, k)
            across(h, k, 0)

    def forward(h, k):
        for s, step in ((0, 1), (1, -1)):
            m = s + 1
            wires.wait(one(h, k, m), base(h) + 4 + 4 * k + s, to(h, 1, step))
            piece = sub(h, origin(h, k, m), s)
            wires.send(piece, piece, base(h) + 6 + 4 * k + s, to(h, 1, step))
            across(h, k, m)

    for h in halves:
        forward(h, 0)
    for h in halves:
        for s, step in ((0, 1), (1, -1)):
            wires.wait(sub(h, origin(h, 3, 0), s), base(h) + 2 + s, to(h, 0, step))
        spread(h, 3)
        across(h, 3, 0)
    for k in (1, 2, 3):
        for h in halves:
            forward(h, k)
    for k in range(4):
        for h in halves:
            for s, step in ((0, 1), (1, -1)):
                wires.wait(
                    sub(h, origin(h, k, 3), s), base(h) + 6 + 4 * k + s, to(h, 1, step)
                )
            across(h, k, 3)
    for k in range(4):
        for m in range(4):
            for h in halves:
                view = full(h, origin(h, k, m, flip=True))
                wires.wait(view, base(h) + 20 + 4 * k + m, place.partner())


def kernel(
    blk, pao_size, cabs_size, pao, cabs, weight, out,
    own, every, part, near, final, held, vals, vnear, vfinal,
    send_a, recv_a, send_b, recv_b, send_c, recv_c, send_d, recv_d, local,
):
    place = Place()
    x = place.x
    load = [
        pltpu.make_async_copy(pao, own.at[pl.ds(0, 48)], local.at[0]),
        pltpu.make_async_copy(cabs, own.at[pl.ds(48, 96)], local.at[1]),
    ] + [
        pltpu.make_async_copy(
            pao.at[:, pl.ds(1920 * h, 1920)], every.at[h, place.me], local.at[2 + h]
        )
        for h in range(2)
    ]
    for copy in load:
        copy.start()
    greet(
        [place.along(a, s) for a in ("y", "z") for s in (1, -1)]
        + [place.partner(), place.beside(1), place.beside(-1)]
    )
    load[0].wait()
    wires = Wires(send_a, recv_a)
    cuts = ((0, 1024), (1024, 896))
    gather_plane(
        place,
        wires,
        lambda h: own.at[pl.ds(0, 48), pl.ds(1920 * h, 1920)],
        lambda h, atom: every.at[h, atom],
        lambda h, atom, s: every.at[h, atom, :, pl.ds(*cuts[s])],
    )
    for copy in load[1:]:
        copy.wait()

    nt = (((1,), (1,)), ((), ()))

    @pl.loop(0, 4)
    def _(line):
        g = None
        for h in range(2):
            rows = every[h, pl.ds(line * 8, 8)].reshape(384, 1920)
            d = lax.dot_general(
                own[:, 1920 * h : 1920 * (h + 1)], rows, nt,
                preferred_element_type=jnp.float32,
            )
            g = d if g is None else g + d
        for c in range(3):
            col = g[:, 128 * c : 128 * c + 128]
            for r in range(6):
                part[line, r * 3 + c] = col[8 * r : 8 * r + 8]
            for k in range(4):
                a, b = 48 + 12 * k, 96 + 12 * k
                at = 18 + line * 3 + c
                part[k, at] = col[a : a + 8]
                part[k, at + 12] = col[b : b + 8]
                part[k, at + 24] = jnp.concatenate(
                    [col[a + 8 : a + 12], col[b + 8 : b + 12]], axis=0
                )

    def klass(step):
        return lax.rem(x + step + 4, 4)

    ring = Wires(send_b, recv_b)
    a, b = pl.ds(0, 27), pl.ds(27, 27)
    left, right = place.beside(-1), place.beside(1)
    ring.send(part.at[klass(2), a], near.at[0], 0, left)
    ring.send(part.at[klass(2), b], near.at[1], 1, right)
    ring.send(part.at[klass(-1), b], final.at[0, b], 2, left)
    ring.send(part.at[klass(1), a], final.at[1, a], 3, right)
    ring.wait(near.at[0], 0, left)
    part[klass(-1), a] = part[klass(-1), a] + near[0]
    ring.send(part.at[klass(-1), a], final.at[0, a], 4, left)
    ring.wait(near.at[1], 1, right)
    part[klass(1), b] = part[klass(1), b] + near[1]
    ring.send(part.at[klass(1), b], final.at[1, b], 5, right)
    ring.wait(final.at[0, b], 2, left)
    ring.wait(final.at[1, a], 3, right)
    ring.wait(final.at[0, a], 4, left)
    ring.wait(final.at[1, b], 5, right)
    w = weight[...].astype(jnp.float32)
    spot = lax.broadcasted_iota(jnp.int32, (8, 48), 1) - 12 * x
    row = lax.broadcasted_iota(jnp.int32, (8, 48), 0)

    def column(b, shift, mask):
        at = jnp.logical_and(mask, spot == row + shift)
        return jnp.where(at, jnp.broadcast_to(w[b : b + 1], (8, 48)), 0.0)

    every_row = row >= 0
    root = [
        jnp.sqrt(jnp.sum(part_w, axis=1, keepdims=True))
        for part_w in (
            column(0, 0, every_row),
            column(1, 0, every_row),
            column(0, 8, row < 4) + column(1, 4, row >= 4),
        )
    ]
    mine = place.me * HELD
    margins, cross = pl.ds(0, 18), pl.ds(18, 36)
    held[pl.ds(mine, 18)] = part[x, margins] + (final[0, margins] + final[1, margins])
    cross_sum = part[x, cross] + (final[0, cross] + final[1, cross])
    for r in range(3):
        held[pl.ds(mine + 18 + 12 * r, 12)] = cross_sum[12 * r : 12 * r + 12] * root[r]

    net = Wires(send_c, recv_c)
    span = ((0, 27), (27, 27))
    pieces = (((0, 14), (14, 13)), ((27, 14), (41, 13)))

    def tiles(atom, start, count):
        return held.at[pl.ds(atom * HELD + start, count)]

    gather_plane(
        place,
        net,
        lambda h: tiles(place.me, *span[h]),
        lambda h, atom: tiles(atom, *span[h]),
        lambda h, atom, s: tiles(atom, *pieces[h][s]),
    )

    lanes = lax.broadcasted_iota(jnp.int32, (8, 128), 1)
    subs = lax.broadcasted_iota(jnp.int32, (8, 128), 0)

    def one_pair(p):
        picks = [blk[l, p] for l in range(4)]
        base = [(b // 2) * HELD for b in picks]
        par = [lax.rem(b, 2) for b in picks]
        acc = [None] * 20
        for l in range(4):
            off = picks[l] * 24
            lt = off // 128
            rem = off - lt * 128
            lm = lt - 3 * x
            hit = jnp.logical_and(lm >= 0, lm < 3)
            lm = jnp.clip(lm, 0, 2)
            turn = lax.rem(24 * l - rem + 128, 128)
            whole = lanes >= rem
            from_here = lanes >= 24 * l
            to_margin = lanes < jnp.where(hit, 24 * l + 24, 0)
            here = jnp.logical_and(from_here, lanes < 24 * l + 24)
            here_margin = jnp.logical_and(from_here, to_margin)

            def place_in(n, two, mask):
                moved = pltpu.roll(jnp.where(whole, two[0], two[1]), turn, 1)
                old = jnp.zeros_like(moved) if acc[n] is None else acc[n]
                acc[n] = jnp.where(mask, moved, old)

            for k in range(4):
                m = held[pl.ds(base[k] + par[k] * 9 + lm, 8)]
                for t in range(3):
                    place_in(3 * k + t, (m[3 * t], m[3 * t + 1]), here_margin)
                c = held[pl.ds(base[k] + 18 + par[k] * 12 + lt, 2)]
                place_in(12 + 2 * k, (c[0], c[1]), here)
                c = held[pl.ds(base[k] + 42 + lt, 2)]
                place_in(13 + 2 * k, (c[0], c[1]), here)
        limit = cabs_size[p] - 12 * x
        for k in range(4):
            first = subs < limit - 48 * k
            low = 4 * par[k]
            second = jnp.logical_and(
                jnp.logical_and(subs >= low, subs < low + 4),
                subs < limit - 48 * k - 8 + low,
            )
            acc[12 + 2 * k] = jnp.where(first, acc[12 + 2 * k], 0.0)
            acc[13 + 2 * k] = jnp.where(second, acc[13 + 2 * k], 0.0)
        margin = jnp.concatenate(acc[:12], axis=0)
        c = jnp.concatenate(acc[12:], axis=0)
        hi = c.astype(jnp.bfloat16)
        lo = (c - hi.astype(jnp.float32)).astype(jnp.bfloat16)
        prod = lax.dot_general(
            jnp.concatenate([hi, lo, hi], axis=0),
            jnp.concatenate([hi, hi, lo], axis=0),
            (((0,), (0,)), ((), ())),
            preferred_element_type=jnp.float32,
        )
        return margin - prod[:96]

    def copy_v(kind, q):
        e, o = 2 * q, 2 * q + 1
        src, dst, device = (
            lambda: (vals.at[klass(2), e], vnear.at[0, q], left),
            lambda: (vals.at[klass(2), o], vnear.at[1, q], right),
            lambda: (vals.at[klass(-1), o], vfinal.at[0, o], left),
            lambda: (vals.at[klass(1), e], vfinal.at[1, e], right),
            lambda: (vals.at[klass(-1), e], vfinal.at[0, e], left),
            lambda: (vals.at[klass(1), o], vfinal.at[1, o], right),
        )[kind]()
        at = kind * 8 + q
        return pltpu.make_async_remote_copy(
            src_ref=src, dst_ref=dst, send_sem=send_d.at[at], recv_sem=recv_d.at[at],
            device_id=device, device_id_type=MESH,
        )

    def second_step(q):
        e, o = 2 * q, 2 * q + 1
        copy_v(0, q).wait_recv()
        vals[klass(-1), e] = vals[klass(-1), e] + vnear[0, q]
        copy_v(4, q).start()
        copy_v(1, q).wait_recv()
        vals[klass(1), o] = vals[klass(1), o] + vnear[1, q]
        copy_v(5, q).start()

    wide = lax.broadcasted_iota(jnp.int32, (96, 128), 1)

    @pl.loop(0, 8)
    def _(q):
        @pl.loop(0, 2)
        def _(half):
            g = 2 * q + half
            v = [one_pair(g * 4 + n) for n in range(4)]
            r1 = pltpu.roll(v[1], 96, 1)
            r2 = pltpu.roll(v[2], 64, 1)
            r3 = pltpu.roll(v[3], 32, 1)
            packed = (
                jnp.where(wide < 96, v[0], r1),
                jnp.where(wide < 64, r1, r2),
                jnp.where(wide < 32, r2, r3),
            )
            for c in range(3):
                for k in range(4):
                    vals[k, g, :, 128 * c : 128 * c + 128] = packed[c][24 * k : 24 * k + 24]

        for kind in range(4):
            copy_v(kind, q).start()

        @pl.when(q > 0)
        def _():
            second_step(q - 1)

    second_step(7)

    narrow = lax.broadcasted_iota(jnp.int32, (24, 128), 1)
    deep = lax.broadcasted_iota(jnp.int32, (24, 128), 0) + 24 * x

    @pl.loop(0, 8)
    def _(q):
        for kind in range(2, 6):
            copy_v(kind, q).wait_recv()
        for half in range(2):
            g = 2 * q + half
            t = vals[x, g] + (vfinal[0, g] + vfinal[1, g])
            t0, t1, t2 = t[:, :128], t[:, 128:256], t[:, 256:]
            v = (
                t0,
                jnp.where(narrow < 32, pltpu.roll(t0, 32, 1), pltpu.roll(t1, 32, 1)),
                jnp.where(narrow < 64, pltpu.roll(t1, 64, 1), pltpu.roll(t2, 64, 1)),
                pltpu.roll(t2, 96, 1),
            )
            for n in range(4):
                size = pao_size[g * 4 + n]
                keep = jnp.logical_and(deep < size, narrow < size)
                out[g * 4 + n] = jnp.where(keep, v[n], 0.0)[:, :96]

    @pl.loop(0, 8)
    def _(q):
        for kind in range(6):
            copy_v(kind, q).wait_send()

    wires.drain()
    ring.drain()
    net.drain()


def fused(blk, pao_size, cabs_size, pao, cabs, weight):
    dma = pltpu.SemaphoreType.DMA
    smem = pl.BlockSpec(memory_space=pltpu.SMEM)
    vmem = pl.BlockSpec(memory_space=pltpu.VMEM)
    hbm = pl.BlockSpec(memory_space=pl.ANY)
    f32 = jnp.float32
    return pl.pallas_call(
        kernel,
        out_shape=jax.ShapeDtypeStruct((64, 24, 96), f32),
        in_specs=[smem, smem, smem, hbm, hbm, vmem],
        out_specs=vmem,
        scratch_shapes=[
            pltpu.VMEM((144, 3840), jnp.bfloat16),
            pltpu.VMEM((2, 32, 48, 1920), jnp.bfloat16),
            pltpu.VMEM((4, TILES, 8, 128), f32),
            pltpu.VMEM((2, 27, 8, 128), f32),
            pltpu.VMEM((2, TILES, 8, 128), f32),
            pltpu.VMEM((32 * HELD, 8, 128), f32),
            pltpu.VMEM((4, 16, 24, 384), f32),
            pltpu.VMEM((2, 8, 24, 384), f32),
            pltpu.VMEM((2, 16, 24, 384), f32),
            dma((2 * PER_HALF,)),
            dma((2 * PER_HALF,)),
            dma((6,)),
            dma((6,)),
            dma((2 * PER_HALF,)),
            dma((2 * PER_HALF,)),
            dma((48,)),
            dma((48,)),
            dma((4,)),
        ],
        compiler_params=pltpu.CompilerParams(
            collective_id=0, has_side_effects=True, vmem_limit_bytes=56 * 1024 * 1024
        ),
        name="fused",
    )(blk, pao_size, cabs_size, pao, cabs, weight)


def shards(pao_blocks, cabs_blocks, cabs_weight, pair_blocks, pao_size, cabs_size):
    return fused(
        pair_blocks.T,
        pao_size,
        cabs_size,
        pao_blocks.reshape(48, -1),
        cabs_blocks.reshape(96, -1),
        cabs_weight,
    )


def solution(mesh):
    placed = (
        P("atom", None, "aux"),
        P("atom", None, "aux"),
        P("atom", None),
        P("atom", None),
        P("atom"),
        P("atom"),
    )
    return jax.shard_map(
        shards, mesh=mesh, in_specs=placed, out_specs=P("atom", "aux", None), check_vma=False
    )
```

```python
import jax
import jax.numpy as jnp
from jax import lax
from jax.experimental import pallas as pl
from jax.experimental.pallas import tpu as pltpu
from jax.sharding import PartitionSpec as P

MESH = pl.DeviceIdType.MESH

PART = 27
HELD = 2 * PART + 1

class Place:
    def __init__(self):
        self.me = lax.axis_index("atom")
        self.x = lax.axis_index("aux")
        self.core = lax.rem(self.me, 2)
        self.z = lax.rem(self.me // 2, 4)
        self.y = self.me // 8

    def atom(self, y=0, z=0, flip=False):
        core = 1 - self.core if flip else self.core
        return (lax.rem(self.y + y + 4, 4) * 4 + lax.rem(self.z + z + 4, 4)) * 2 + core

    def along(self, axis, step):
        at = self.atom(**{axis: step})
        return (at, self.x)

    def partner(self):
        return (self.atom(flip=True), self.x)

    def beside(self, step):
        return (self.me, lax.rem(self.x + step + 4, 4))


def greet(devices):
    barrier = pltpu.get_barrier_semaphore()
    for device in devices:
        pl.semaphore_signal(barrier, inc=1, device_id=device, device_id_type=MESH)
    pl.semaphore_wait(barrier, len(devices))


class Wires:
    def __init__(self, send_sem, recv_sem, first=0):
        self.send_sem, self.recv_sem, self.first = send_sem, recv_sem, first

    def copy(self, src, dst, at, device):
        return pltpu.make_async_remote_copy(
            src_ref=src,
            dst_ref=dst,
            send_sem=self.send_sem,
            recv_sem=self.recv_sem.at[self.first + at],
            device_id=device,
            device_id_type=MESH,
        )

    def send(self, src, dst, at, device):
        self.copy(src, dst, at, device).start()

    def wait(self, view, at, device):
        self.copy(view, view, at, device).wait_recv()

    def drain(self, view, device):
        self.copy(view, view, 0, device).wait_send()


OFFSETS = (0, -1, 1, 2)
AXES = (("z", "y"), ("y", "z"))


class Gather:
    BASE = 15
    TOTAL = 2 * BASE

    def __init__(self, place, wires, own, full, sub, group):
        self.place, self.wires, self.own = place, wires, own
        self.full, self.sub, self.group = full, sub, group

    def origin(self, h, k, m):
        first, second = AXES[h]
        return self.place.atom(**{first: OFFSETS[k], second: OFFSETS[m]})

    def chunk(self, h, k, m):
        return self.full(h, self.origin(h, k, m))

    def to(self, h, order, step):
        return self.place.along(AXES[h][order], step)

    def source(self, h, k, m):
        return self.own(h) if (k, m) == (0, 0) else self.chunk(h, k, m)

    def across(self, h, k, m):
        self.wires.send(
            self.source(h, k, m), self.chunk(h, k, m),
            self.TOTAL + self.group(h, k, m), self.place.partner(),
        )

    def spread(self, h, k):
        src, dst = self.source(h, k, 0), self.chunk(h, k, 0)
        at = self.BASE * h + 3 + 3 * k
        self.wires.send(src, dst, at, self.to(h, 1, 1))
        self.wires.send(src, dst, at + 1, self.to(h, 1, -1))

    def start(self):
        for h in (0, 1):
            at = self.BASE * h
            self.wires.send(self.own(h), self.chunk(h, 0, 0), at, self.to(h, 0, 1))
            self.wires.send(self.own(h), self.chunk(h, 0, 0), at + 1, self.to(h, 0, -1))
        for h in (0, 1):
            self.spread(h, 0)
            self.across(h, 0, 0)

    def hop1(self, h):
        for s, step in ((0, 1), (1, -1)):
            self.wires.wait(self.chunk(h, s + 1, 0), self.BASE * h + s, self.to(h, 0, step))

    def relay1(self, h):
        for s, step in ((0, 1), (1, -1)):
            piece = self.sub(h, self.origin(h, s + 1, 0), s)
            self.wires.send(piece, piece, self.BASE * h + 2, self.to(h, 0, step))

    def last1(self, h):
        self.wires.wait(self.chunk(h, 3, 0), self.BASE * h + 2, self.to(h, 0, 1))

    def hop2(self, h, k):
        at = self.BASE * h + 3 + 3 * k
        for s, step in ((0, 1), (1, -1)):
            self.wires.wait(self.chunk(h, k, s + 1), at + s, self.to(h, 1, step))

    def relay2(self, h, k):
        at = self.BASE * h + 5 + 3 * k
        for s, step in ((0, 1), (1, -1)):
            piece = self.sub(h, self.origin(h, k, s + 1), s)
            self.wires.send(piece, piece, at, self.to(h, 1, step))
        for s in (0, 1):
            self.across(h, k, s + 1)

    def last2(self, h, k):
        self.wires.wait(
            self.chunk(h, k, 3), self.BASE * h + 5 + 3 * k, self.to(h, 1, 1)
        )
        self.across(h, k, 3)

    def step_a(self):
        for h in (0, 1):
            self.hop1(h)
            self.relay1(h)
        for h in (0, 1):
            for k in (1, 2):
                self.spread(h, k)
                self.across(h, k, 0)

    def step_b(self):
        for h in (0, 1):
            self.hop2(h, 0)
            self.relay2(h, 0)

    def step_c(self):
        for h in (0, 1):
            self.last1(h)
            self.spread(h, 3)
            self.across(h, 3, 0)

    def step_d(self, k):
        for h in (0, 1):
            self.hop2(h, k)
            self.relay2(h, k)

    def step_e(self):
        for k in range(4):
            for h in (0, 1):
                self.last2(h, k)


class RingSum:
    def __init__(self, place, wires, part, near, final):
        self.place, self.wires = place, wires
        self.part, self.near, self.final = part, near, final
        self.left, self.right = place.beside(-1), place.beside(1)

    def klass(self, step):
        return lax.rem(self.place.x + step + 4, 4)

    def begin(self):
        a, b = pl.ds(0, 14), pl.ds(14, 13)
        send, part = self.wires.send, self.part
        send(part(self.klass(2), a), self.near.at[0, a], 0, self.left)
        send(part(self.klass(2), b), self.near.at[1, pl.ds(0, 13)], 1, self.right)
        send(part(self.klass(-1), b), self.final.at[0, b], 2, self.left)
        send(part(self.klass(1), a), self.final.at[1, a], 2, self.right)

    def middle(self):
        a, b = pl.ds(0, 14), pl.ds(14, 13)
        self.wires.wait(self.near.at[0, a], 0, self.left)
        mine = self.part(self.klass(-1), a)
        mine[...] = mine[...] + self.near[0]
        self.wires.send(mine, self.final.at[0, a], 2, self.left)
        self.wires.wait(self.near.at[1, pl.ds(0, 13)], 1, self.right)
        mine = self.part(self.klass(1), b)
        mine[...] = mine[...] + self.near[1, 0:13]
        self.wires.send(mine, self.final.at[1, b], 2, self.right)

    def finish(self):
        self.wires.wait(self.final, 2, self.left)
        own = self.part(self.place.x, pl.ds(0, PART))
        return own[...] + (self.final[0] + self.final[1])


def kernel(
    blk, pao_size, cabs_size, pao, cabs, weight, out,
    own, every, parts, near, final, held, vals, vnear, vfinal,
    send_a, recv_a, send_b, recv_b, send_c, recv_c, send_v, recv_v, local,
):
    place = Place()
    x = place.x
    load = [
        pltpu.make_async_copy(pao, own.at[pl.ds(0, 48)], local.at[0]),
        pltpu.make_async_copy(cabs, own.at[pl.ds(48, 96)], local.at[1]),
    ] + [
        pltpu.make_async_copy(
            pao.at[:, pl.ds(1920 * h, 1920)], every.at[32 * h + place.me], local.at[2 + h]
        )
        for h in range(2)
    ]
    for copy in load:
        copy.start()
    greet(
        [place.along(a, s) for a in ("y", "z") for s in (1, -1)]
        + [place.partner(), place.beside(1), place.beside(-1)]
    )
    load[0].wait()
    cuts = ((0, 1024), (1024, 896))
    first = Gather(
        place,
        Wires(send_a, recv_a),
        lambda h: own.at[pl.ds(0, 48), pl.ds(1920 * h, 1920)],
        lambda h, atom: every.at[32 * h + atom],
        lambda h, atom, s: every.at[32 * h + atom, :, pl.ds(*cuts[s])],
        lambda h, k, m: m if h == 0 else k,
    )
    sums = [
        RingSum(
            place,
            Wires(send_b.at[r], recv_b, 3 * r),
            lambda k, span, r=r: parts.at[r, k, span],
            near.at[r],
            final.at[r],
        )
        for r in range(2)
    ]

    def tiles(atom, start, count):
        return held.at[pl.ds(atom * HELD + start, count)]

    span = ((0, 14), (14, 13))
    pieces = (((0, 7), (7, 7)), ((14, 7), (21, 6)))
    nets = [
        Gather(
            place,
            Wires(send_c.at[r], recv_c, 31 * r),
            lambda h, r=r: tiles(place.me, PART * r + span[h][0], span[h][1]),
            lambda h, atom, r=r: tiles(atom, PART * r + span[h][0], span[h][1]),
            lambda h, atom, s, r=r: tiles(
                atom, PART * r + pieces[h][s][0], pieces[h][s][1]
            ),
            lambda h, k, m: 0,
        )
        for r in range(2)
    ]

    first.start()

    w = weight[...].astype(jnp.float32)
    spot = lax.broadcasted_iota(jnp.int32, (8, 48), 1) - 12 * x
    row = lax.broadcasted_iota(jnp.int32, (8, 48), 0)

    def column(b, shift, mask):
        at = jnp.logical_and(mask, spot == row + shift)
        return jnp.where(at, jnp.broadcast_to(w[b : b + 1], (8, 48)), 0.0)

    root = [
        jnp.sqrt(jnp.sum(part_w, axis=1, keepdims=True))
        for part_w in (
            column(0, 0, row >= 0),
            column(1, 0, row >= 0),
            column(0, 8, row < 4) + column(1, 4, row >= 4),
        )
    ]

    nt = (((1,), (1,)), ((), ()))

    def line_products(step, slot):
        line = lax.rem(place.y + step + 4, 4)
        first.wires.wait(every.at[pl.ds(0, 8)], first.TOTAL + OFFSETS.index(step), place.partner())
        g = None
        for h in range(2):
            rows = every[pl.ds(32 * h + line * 8, 8)].reshape(384, 1920)
            d = lax.dot_general(
                own[:, 1920 * h : 1920 * (h + 1)], rows, nt,
                preferred_element_type=jnp.float32,
            )
            g = d if g is None else g + d
        r, start = (0, 9 * slot) if slot < 3 else (1, 0)
        for c in range(3):
            col = g[:, 128 * c : 128 * c + 128]
            for t in range(6):
                parts[1, line, 9 + t * 3 + c] = col[8 * t : 8 * t + 8]
            for k in range(4):
                a, b = 48 + 12 * k, 96 + 12 * k
                parts[r, k, start + c] = col[a : a + 8]
                parts[r, k, start + 3 + c] = col[b : b + 8]
                parts[r, k, start + 6 + c] = jnp.concatenate(
                    [col[a + 8 : a + 12], col[b + 8 : b + 12]], axis=0
                )

    mine = place.me * HELD

    def keep_part(r):
        total = sums[r].finish()
        for n in range(9):
            if r == 0 or n < 3:
                held[pl.ds(mine + PART * r + 3 * n, 3)] = total[3 * n : 3 * n + 3] * root[n % 3]
        if r == 1:
            held[pl.ds(mine + PART + 9, 18)] = total[9:]

    first.hop1(0)
    first.relay1(0)
    for k in (1, 2):
        first.spread(0, k)
        first.across(0, k, 0)
    first.hop1(1)
    for k in (1, 2):
        first.spread(1, k)
        first.across(1, k, 0)
    first.last1(0)
    first.spread(0, 3)
    first.across(0, 3, 0)
    first.relay1(1)
    first.hop2(1, 0)
    first.relay2(1, 0)
    for copy in load[1:]:
        copy.wait()
    first.hop2(0, 0)
    first.relay2(0, 0)
    for k in (1, 2):
        first.hop2(1, k)
        first.relay2(1, k)
        first.hop2(0, k)
        first.relay2(0, k)
    first.last2(1, 0)
    line_products(0, 0)
    first.last1(1)
    first.spread(1, 3)
    first.across(1, 3, 0)
    first.hop2(0, 3)
    first.relay2(0, 3)
    first.last2(1, 1)
    first.last2(1, 2)
    line_products(1, 1)
    line_products(-1, 2)
    sums[0].begin()
    first.last2(0, 0)
    first.hop2(1, 3)
    first.relay2(1, 3)
    first.last2(0, 1)
    first.last2(0, 2)
    sums[0].middle()
    first.last2(0, 3)
    first.last2(1, 3)
    keep_part(0)
    nets[0].start()
    line_products(2, 3)
    sums[1].begin()
    nets[0].step_a()
    sums[1].middle()
    nets[0].step_b()
    nets[0].step_c()
    keep_part(1)
    nets[1].start()
    nets[0].step_d(1)
    nets[0].step_d(2)
    nets[1].step_a()
    nets[0].step_d(3)
    nets[1].step_b()
    nets[1].step_c()
    nets[0].step_e()
    for k in (1, 2, 3):
        nets[1].step_d(k)
    nets[1].step_e()
    for r in range(2):
        nets[r].wires.wait(held.at[pl.ds(0, 16 * PART)], nets[r].TOTAL, place.partner())

    lanes = lax.broadcasted_iota(jnp.int32, (8, 128), 1)
    subs = lax.broadcasted_iota(jnp.int32, (8, 128), 0)

    def half_of(n, bits):
        return lax.shift_right_logical(n, jnp.int32(bits))

    def one_pair(p):
        picks = [blk[l, p] for l in range(4)]
        base = [half_of(b, 1) * HELD for b in picks]
        par = [jnp.bitwise_and(b, 1) for b in picks]
        lines = [half_of(b, 4) for b in picks]
        acc = [None] * 20
        for l in range(4):
            off = jnp.bitwise_and(picks[l], 15) * 24
            u = half_of(off, 7)
            rem = jnp.bitwise_and(off, 127)
            turn = jnp.bitwise_and(24 * l + 128 - rem, 127)
            whole = lanes >= rem
            from_here = lanes >= 24 * l
            to_margin = lanes < jnp.where(lines[l] == x, 24 * l + 24, 0)
            here = jnp.logical_and(from_here, lanes < 24 * l + 24)
            here_margin = jnp.logical_and(from_here, to_margin)

            def place_in(n, two, mask):
                moved = pltpu.roll(jnp.where(whole, two[0], two[1]), turn, 1)
                old = jnp.zeros_like(moved) if acc[n] is None else acc[n]
                acc[n] = jnp.where(mask, moved, old)

            for k in range(4):
                m = held[pl.ds(base[k] + par[k] * 9 + (u + PART + 9), 8)]
                for t in range(3):
                    place_in(3 * k + t, (m[3 * t], m[3 * t + 1]), here_margin)
                away = jnp.bitwise_and(lines[l] - lines[k], 3)
                at = base[k] + jnp.bitwise_xor(away, half_of(away, 1)) * 9 + u
                c = held[pl.ds(at + par[k] * 3, 2)]
                place_in(12 + 2 * k, (c[0], c[1]), here)
                c = held[pl.ds(at + 6, 2)]
                place_in(13 + 2 * k, (c[0], c[1]), here)
        limit = cabs_size[p] - 12 * x
        for k in range(4):
            first = subs < limit - 48 * k
            low = 4 * par[k]
            second = jnp.logical_and(
                jnp.logical_and(subs >= low, subs < low + 4),
                subs < limit - 48 * k - 8 + low,
            )
            acc[12 + 2 * k] = jnp.where(first, acc[12 + 2 * k], 0.0)
            acc[13 + 2 * k] = jnp.where(second, acc[13 + 2 * k], 0.0)
        margin = jnp.concatenate(acc[:12], axis=0)
        c = jnp.concatenate(acc[12:], axis=0)
        hi = c.astype(jnp.bfloat16)
        lo = (c - hi.astype(jnp.float32)).astype(jnp.bfloat16)
        prod = lax.dot_general(
            jnp.concatenate([hi, lo, hi], axis=0),
            jnp.concatenate([hi, hi, lo], axis=0),
            (((0,), (0,)), ((), ())),
            preferred_element_type=jnp.float32,
        )
        return margin - prod[:96]

    left, right = place.beside(-1), place.beside(1)
    klass = sums[0].klass

    def copy_v(kind, q):
        e, o = 2 * q, 2 * q + 1
        src, dst, device, at = (
            lambda: (vals.at[klass(2) * 16 + e], vnear.at[2 * q], left, 3 * q),
            lambda: (vals.at[klass(2) * 16 + o], vnear.at[2 * q + 1], right, 3 * q + 1),
            lambda: (vals.at[klass(-1) * 16 + o], vfinal.at[o], left, 3 * q + 2),
            lambda: (vals.at[klass(1) * 16 + e], vfinal.at[16 + e], right, 3 * q + 2),
            lambda: (vals.at[klass(-1) * 16 + e], vfinal.at[e], left, 3 * q + 2),
            lambda: (vals.at[klass(1) * 16 + o], vfinal.at[16 + o], right, 3 * q + 2),
        )[kind]()
        return Wires(send_v, recv_v).copy(src, dst, at, device)

    def second_step(q):
        e, o = klass(-1) * 16 + 2 * q, klass(1) * 16 + 2 * q + 1
        copy_v(0, q).wait_recv()
        vals[e] = vals[e] + vnear[2 * q]
        copy_v(4, q).start()
        copy_v(1, q).wait_recv()
        vals[o] = vals[o] + vnear[2 * q + 1]
        copy_v(5, q).start()

    wide = lax.broadcasted_iota(jnp.int32, (96, 128), 1)

    @pl.loop(0, 8)
    def _(q):
        @pl.loop(0, 2)
        def _(half):
            g = 2 * q + half
            v = [one_pair(g * 4 + n) for n in range(4)]
            r1 = pltpu.roll(v[1], 96, 1)
            r2 = pltpu.roll(v[2], 64, 1)
            r3 = pltpu.roll(v[3], 32, 1)
            packed = (
                jnp.where(wide < 96, v[0], r1),
                jnp.where(wide < 64, r1, r2),
                jnp.where(wide < 32, r2, r3),
            )
            for c in range(3):
                for k in range(4):
                    vals[k * 16 + g, :, 128 * c : 128 * c + 128] = packed[c][24 * k : 24 * k + 24]

        for kind in range(4):
            copy_v(kind, q).start()

        @pl.when(q > 0)
        def _():
            second_step(q - 1)

    second_step(7)

    narrow = lax.broadcasted_iota(jnp.int32, (24, 128), 1)
    deep = lax.broadcasted_iota(jnp.int32, (24, 128), 0) + 24 * x

    @pl.loop(0, 8)
    def _(q):
        view = vfinal.at[pl.ds(0, 4)]
        Wires(send_v, recv_v).wait(view, 3 * q + 2, left)
        for half in range(2):
            g = 2 * q + half
            t = vals[x * 16 + g] + (vfinal[g] + vfinal[16 + g])
            t0, t1, t2 = t[:, :128], t[:, 128:256], t[:, 256:]
            v = (
                t0,
                jnp.where(narrow < 32, pltpu.roll(t0, 32, 1), pltpu.roll(t1, 32, 1)),
                jnp.where(narrow < 64, pltpu.roll(t1, 64, 1), pltpu.roll(t2, 64, 1)),
                pltpu.roll(t2, 96, 1),
            )
            for n in range(4):
                size = pao_size[g * 4 + n]
                keep = jnp.logical_and(deep < size, narrow < size)
                out[g * 4 + n] = jnp.where(keep, v[n], 0.0)[:, :96]

    first.wires.drain(every.at[pl.ds(0, 62)], left)
    for r in range(2):
        sums[r].wires.drain(held.at[pl.ds(0, 3 * PART)], left)
        nets[r].wires.drain(held.at[pl.ds(0, 31 * PART)], left)
    Wires(send_v, recv_v).drain(vals.at[pl.ds(0, 48)], left)


def fused(blk, pao_size, cabs_size, pao, cabs, weight):
    dma = pltpu.SemaphoreType.DMA
    smem = pl.BlockSpec(memory_space=pltpu.SMEM)
    vmem = pl.BlockSpec(memory_space=pltpu.VMEM)
    hbm = pl.BlockSpec(memory_space=pl.ANY)
    f32 = jnp.float32
    return pl.pallas_call(
        kernel,
        out_shape=jax.ShapeDtypeStruct((64, 24, 96), f32),
        in_specs=[smem, smem, smem, hbm, hbm, vmem],
        out_specs=vmem,
        scratch_shapes=[
            pltpu.VMEM((144, 3840), jnp.bfloat16),
            pltpu.VMEM((64, 48, 1920), jnp.bfloat16),
            pltpu.VMEM((2, 4, PART, 8, 128), f32),
            pltpu.VMEM((2, 2, 14, 8, 128), f32),
            pltpu.VMEM((2, 2, PART, 8, 128), f32),
            pltpu.VMEM((32 * HELD, 8, 128), f32),
            pltpu.VMEM((64, 24, 384), f32),
            pltpu.VMEM((16, 24, 384), f32),
            pltpu.VMEM((32, 24, 384), f32),
            dma,
            dma((Gather.TOTAL + 4,)),
            dma((2,)),
            dma((6,)),
            dma((2,)),
            dma((2 * Gather.TOTAL + 2,)),
            dma,
            dma((24,)),
            dma((4,)),
        ],
        compiler_params=pltpu.CompilerParams(
            collective_id=0, has_side_effects=True, vmem_limit_bytes=56 * 1024 * 1024
        ),
        name="fused",
    )(blk, pao_size, cabs_size, pao, cabs, weight)


def shards(pao_blocks, cabs_blocks, cabs_weight, pair_blocks, pao_size, cabs_size):
    return fused(
        pair_blocks.T,
        pao_size,
        cabs_size,
        pao_blocks.reshape(48, -1),
        cabs_blocks.reshape(96, -1),
        cabs_weight,
    )


def solution(mesh):
    placed = (
        P("atom", None, "aux"),
        P("atom", None, "aux"),
        P("atom", None),
        P("atom", None),
        P("atom"),
        P("atom"),
    )
    return jax.shard_map(
        shards, mesh=mesh, in_specs=placed, out_specs=P("atom", "aux", None), check_vma=False
    )
```

```python
import jax
import jax.numpy as jnp
from jax import lax
from jax.experimental import pallas as pl
from jax.experimental.pallas import tpu as pltpu
from jax.sharding import PartitionSpec as P

MESH = pl.DeviceIdType.MESH

PARTS = (((0, 2), 0, 18), ((1,), 18, 9), ((3,), 27, 9), )
HELD = 37
CHOSEN = 577

START, RELAY, SPREAD, PASS, ACROSS, LINE = range(6)
FAR, PLAIN, MIXED, KEEP, PICK, BLOCK = range(6, 12)

ORDER = (
    (START, 0, 0, 0), (START, 0, 0, 1), (START, 0, 1, 0), (START, 0, 1, 1),
    (ACROSS, 0, 1, 0, 0), (ACROSS, 0, 0, 0, 0), (SPREAD, 0, 1, 0, 0),
    (SPREAD, 0, 1, 0, 1), (SPREAD, 0, 0, 0, 0), (SPREAD, 0, 0, 0, 1),
    (ACROSS, 0, 1, 2, 0), (ACROSS, 0, 1, 1, 0), (ACROSS, 0, 0, 1, 0), (RELAY, 0, 0, 0),
    (RELAY, 0, 0, 1), (RELAY, 0, 1, 0), (RELAY, 0, 1, 1), (ACROSS, 0, 0, 2, 0),
    (SPREAD, 0, 1, 2, 0), (SPREAD, 0, 1, 2, 1), (SPREAD, 0, 0, 1, 0),
    (SPREAD, 0, 0, 2, 1), (ACROSS, 0, 1, 0, 1), (ACROSS, 0, 1, 0, 2),
    (ACROSS, 0, 0, 0, 2), (ACROSS, 0, 0, 0, 1), (ACROSS, 0, 1, 3, 0),
    (ACROSS, 0, 0, 3, 0), (PASS, 0, 1, 0, 0), (PASS, 0, 1, 0, 1), (PASS, 0, 0, 0, 0),
    (SPREAD, 0, 0, 3, 1), (SPREAD, 0, 1, 1, 0), (SPREAD, 0, 1, 1, 1),
    (SPREAD, 0, 0, 3, 0), (ACROSS, 0, 1, 2, 2), (ACROSS, 0, 0, 2, 2),
    (ACROSS, 0, 0, 1, 1), (SPREAD, 0, 0, 1, 1), (ACROSS, 0, 1, 2, 1),
    (ACROSS, 0, 1, 0, 3), (PASS, 0, 1, 2, 0), (PASS, 0, 1, 2, 1), (SPREAD, 0, 0, 2, 0),
    (ACROSS, 0, 0, 3, 2), (LINE, 0), (SPREAD, 0, 1, 3, 0), (SPREAD, 0, 1, 3, 1),
    (PASS, 0, 0, 0, 1), (PICK, 0), (ACROSS, 0, 1, 1, 1), (ACROSS, 0, 1, 1, 2),
    (ACROSS, 0, 0, 3, 1), (PASS, 0, 0, 1, 0), (PASS, 0, 0, 3, 1), (ACROSS, 0, 1, 2, 3),
    (ACROSS, 0, 0, 1, 2), (PASS, 0, 1, 1, 0), (PASS, 0, 1, 1, 1), (PASS, 0, 0, 3, 0),
    (PASS, 0, 0, 1, 1), (ACROSS, 0, 0, 0, 3), (LINE, 2), (ACROSS, 0, 0, 2, 1),
    (PLAIN, 0, 1), (FAR, 0, 0), (PASS, 0, 0, 2, 0), (PASS, 0, 0, 2, 1), (PICK, 2),
    (PASS, 0, 1, 3, 0), (PASS, 0, 1, 3, 1), (ACROSS, 0, 1, 3, 2), (FAR, 0, 1),
    (PLAIN, 0, 0), (ACROSS, 0, 1, 3, 1), (ACROSS, 0, 1, 1, 3), (MIXED, 0, 0),
    (ACROSS, 0, 0, 3, 3), (MIXED, 0, 1), (ACROSS, 0, 0, 1, 3), (LINE, 1),
    (ACROSS, 0, 0, 2, 3), (FAR, 1, 1), (FAR, 1, 0), (ACROSS, 0, 1, 3, 3),
    (PLAIN, 1, 1), (PLAIN, 1, 0), (PICK, 1), (BLOCK, 0, 0), (BLOCK, 0, 1),
    (KEEP, 0), (SPREAD, 1, 1, 0, 0), (START, 1, 0, 1), (START, 1, 1, 0),
    (START, 1, 1, 1), (ACROSS, 1, 0, 0, 0), (LINE, 3), (ACROSS, 1, 1, 0, 0),
    (FAR, 2, 1), (FAR, 2, 0), (START, 1, 0, 0), (SPREAD, 1, 1, 0, 1),
    (SPREAD, 1, 0, 0, 0), (SPREAD, 1, 0, 0, 1), (PLAIN, 2, 1), (MIXED, 1, 0),
    (MIXED, 1, 1), (PLAIN, 2, 0), (PICK, 3), (BLOCK, 1, 0), (BLOCK, 1, 1),
    (SPREAD, 1, 1, 2, 0), (RELAY, 1, 0, 1), (RELAY, 1, 1, 0), (RELAY, 1, 1, 1),
    (ACROSS, 1, 1, 1, 0), (ACROSS, 1, 1, 2, 0), (ACROSS, 1, 1, 0, 1),
    (ACROSS, 1, 0, 2, 0), (MIXED, 2, 1), (MIXED, 2, 0), (SPREAD, 1, 1, 1, 1),
    (SPREAD, 1, 0, 2, 0), (SPREAD, 1, 0, 2, 1), (RELAY, 1, 0, 0), (ACROSS, 1, 0, 1, 0),
    (ACROSS, 1, 0, 0, 2), (ACROSS, 1, 1, 0, 2), (ACROSS, 1, 0, 0, 1), (KEEP, 1),
    (SPREAD, 1, 1, 1, 0), (SPREAD, 1, 1, 2, 1), (SPREAD, 1, 0, 1, 0),
    (SPREAD, 1, 0, 1, 1), (ACROSS, 2, 0, 0, 0), (ACROSS, 2, 1, 0, 0), (START, 2, 0, 0),
    (START, 2, 0, 1), (START, 2, 1, 0), (START, 2, 1, 1), (SPREAD, 2, 0, 0, 0),
    (SPREAD, 2, 0, 0, 1), (SPREAD, 2, 1, 0, 0), (SPREAD, 2, 1, 0, 1), (BLOCK, 2, 0),
    (BLOCK, 2, 1), (ACROSS, 1, 1, 3, 0), (SPREAD, 1, 1, 3, 0), (SPREAD, 1, 1, 3, 1),
    (PASS, 1, 0, 0, 0), (PASS, 1, 0, 0, 1), (KEEP, 2), (ACROSS, 1, 1, 2, 1),
    (START, 3, 1, 0), (START, 3, 1, 1), (ACROSS, 3, 0, 0, 0), (ACROSS, 3, 1, 0, 0),
    (ACROSS, 1, 1, 1, 2), (START, 3, 0, 0), (START, 3, 0, 1), (SPREAD, 1, 0, 3, 0),
    (SPREAD, 1, 0, 3, 1), (ACROSS, 1, 0, 3, 0), (ACROSS, 1, 0, 2, 1),
    (ACROSS, 1, 0, 2, 2), (SPREAD, 3, 1, 0, 0), (SPREAD, 3, 1, 0, 1), (BLOCK, 3, 0),
    (ACROSS, 1, 0, 1, 1), (PASS, 1, 1, 1, 0), (PASS, 1, 1, 2, 1), (SPREAD, 3, 0, 0, 0),
    (SPREAD, 3, 0, 0, 1), (ACROSS, 1, 0, 1, 2), (ACROSS, 1, 1, 2, 2),
    (ACROSS, 2, 1, 1, 0), (ACROSS, 2, 1, 2, 0), (RELAY, 2, 0, 0), (RELAY, 2, 0, 1),
    (ACROSS, 2, 0, 2, 0), (RELAY, 2, 1, 0), (RELAY, 2, 1, 1), (ACROSS, 2, 0, 1, 0),
    (ACROSS, 1, 1, 1, 1), (SPREAD, 2, 1, 1, 0), (SPREAD, 2, 1, 2, 1),
    (SPREAD, 2, 0, 2, 0), (SPREAD, 2, 0, 1, 1), (ACROSS, 2, 0, 0, 1),
    (ACROSS, 2, 0, 0, 2), (ACROSS, 2, 1, 0, 1), (ACROSS, 2, 1, 0, 2),
    (SPREAD, 2, 1, 2, 0), (SPREAD, 2, 1, 1, 1), (SPREAD, 2, 0, 1, 0),
    (SPREAD, 2, 0, 2, 1), (BLOCK, 3, 1), (ACROSS, 1, 0, 0, 3), (PASS, 1, 1, 0, 0),
    (PASS, 1, 1, 1, 1), (ACROSS, 1, 1, 3, 1), (PASS, 1, 0, 1, 0), (PASS, 1, 0, 2, 1),
    (ACROSS, 1, 1, 3, 2), (SPREAD, 3, 1, 1, 0), (SPREAD, 3, 1, 1, 1),
    (ACROSS, 3, 1, 2, 0), (ACROSS, 3, 1, 1, 0), (RELAY, 3, 1, 0), (RELAY, 3, 1, 1),
    (ACROSS, 3, 0, 1, 0), (ACROSS, 3, 0, 2, 0), (RELAY, 3, 0, 0), (RELAY, 3, 0, 1),
    (SPREAD, 3, 0, 1, 0), (SPREAD, 3, 0, 1, 1), (SPREAD, 3, 1, 2, 0),
    (SPREAD, 3, 1, 2, 1), (ACROSS, 3, 1, 0, 1), (ACROSS, 1, 0, 3, 1),
    (ACROSS, 1, 0, 3, 2), (SPREAD, 3, 0, 2, 0), (SPREAD, 3, 0, 2, 1),
    (ACROSS, 3, 1, 0, 2), (PASS, 3, 1, 0, 0), (PASS, 3, 1, 0, 1), (BLOCK, 0, 2),
    (ACROSS, 3, 0, 0, 1), (PASS, 1, 1, 3, 0), (PASS, 1, 1, 0, 1), (ACROSS, 3, 0, 0, 2),
    (ACROSS, 2, 0, 3, 0), (PASS, 3, 0, 0, 0), (PASS, 3, 0, 0, 1), (ACROSS, 2, 1, 3, 0),
    (SPREAD, 2, 0, 3, 0), (SPREAD, 2, 0, 3, 1), (SPREAD, 2, 1, 3, 0),
    (SPREAD, 2, 1, 3, 1), (ACROSS, 2, 1, 2, 2), (ACROSS, 2, 1, 1, 1),
    (ACROSS, 2, 0, 2, 1), (ACROSS, 2, 0, 1, 2), (PASS, 1, 1, 2, 0), (PASS, 1, 1, 3, 1),
    (ACROSS, 2, 1, 2, 1), (PASS, 1, 0, 3, 0), (PASS, 1, 0, 3, 1), (ACROSS, 2, 1, 1, 2),
    (ACROSS, 2, 0, 1, 1), (ACROSS, 2, 0, 2, 2), (PASS, 2, 1, 1, 0), (PASS, 2, 1, 1, 1),
    (BLOCK, 1, 2), (ACROSS, 1, 1, 1, 3), (PASS, 1, 0, 2, 0), (PASS, 1, 0, 1, 1),
    (PASS, 2, 1, 2, 0), (PASS, 2, 1, 2, 1), (PASS, 2, 1, 0, 0), (PASS, 2, 1, 0, 1),
    (ACROSS, 3, 1, 1, 1), (ACROSS, 3, 1, 3, 0), (PASS, 2, 0, 0, 0), (PASS, 2, 0, 0, 1),
    (ACROSS, 3, 1, 1, 2), (PASS, 3, 1, 1, 0), (PASS, 3, 1, 1, 1), (ACROSS, 3, 0, 3, 0),
    (SPREAD, 3, 0, 3, 0), (SPREAD, 3, 0, 3, 1), (SPREAD, 3, 1, 3, 0),
    (SPREAD, 3, 1, 3, 1), (ACROSS, 3, 0, 1, 2), (ACROSS, 3, 0, 1, 1),
    (ACROSS, 3, 1, 2, 1), (PASS, 3, 1, 2, 0), (PASS, 3, 1, 2, 1), (ACROSS, 3, 1, 2, 2),
    (PASS, 3, 0, 1, 0), (PASS, 3, 0, 1, 1), (ACROSS, 3, 1, 0, 3), (ACROSS, 3, 0, 2, 1),
    (PASS, 3, 0, 2, 0), (PASS, 3, 0, 2, 1), (ACROSS, 3, 0, 2, 2), (BLOCK, 2, 2),
    (ACROSS, 3, 0, 0, 3), (PASS, 2, 0, 2, 0), (PASS, 2, 0, 1, 1), (ACROSS, 1, 1, 0, 3),
    (PASS, 2, 0, 1, 0), (PASS, 2, 0, 2, 1), (PASS, 2, 1, 3, 0), (PASS, 2, 1, 3, 1),
    (ACROSS, 2, 1, 3, 1), (ACROSS, 2, 1, 3, 2), (PASS, 2, 0, 3, 0), (PASS, 2, 0, 3, 1),
    (ACROSS, 2, 0, 3, 2), (ACROSS, 2, 0, 3, 1), (ACROSS, 1, 1, 2, 3),
    (ACROSS, 1, 0, 3, 3), (ACROSS, 1, 1, 3, 3), (BLOCK, 3, 2), (ACROSS, 2, 1, 2, 3),
    (ACROSS, 2, 1, 1, 3), (ACROSS, 1, 0, 1, 3), (ACROSS, 1, 0, 2, 3),
    (ACROSS, 2, 0, 0, 3), (ACROSS, 3, 1, 1, 3), (ACROSS, 2, 1, 0, 3), (BLOCK, 4, 0),
    (PASS, 3, 1, 3, 0), (PASS, 3, 1, 3, 1), (ACROSS, 3, 1, 3, 1), (ACROSS, 3, 1, 3, 2),
    (PASS, 3, 0, 3, 0), (PASS, 3, 0, 3, 1), (ACROSS, 3, 0, 3, 1), (ACROSS, 3, 0, 3, 2),
    (ACROSS, 3, 1, 2, 3), (ACROSS, 3, 0, 1, 3), (ACROSS, 3, 0, 2, 3), (BLOCK, 4, 1),
    (ACROSS, 2, 0, 2, 3), (ACROSS, 2, 0, 1, 3), (ACROSS, 2, 1, 3, 3),
    (ACROSS, 2, 0, 3, 3), (BLOCK, 4, 2), (BLOCK, 5, 0), (ACROSS, 3, 1, 3, 3),
    (ACROSS, 3, 0, 3, 3), (BLOCK, 5, 1), (BLOCK, 5, 2),
)


class Place:
    def __init__(self):
        self.me = lax.axis_index("atom")
        self.x = lax.axis_index("aux")
        self.core = lax.rem(self.me, 2)
        self.z = lax.rem(self.me // 2, 4)
        self.y = self.me // 8

    def atom(self, y=0, z=0, flip=False):
        core = 1 - self.core if flip else self.core
        return (lax.rem(self.y + y + 4, 4) * 4 + lax.rem(self.z + z + 4, 4)) * 2 + core

    def along(self, axis, step):
        at = self.atom(**{axis: step})
        return (at, self.x)

    def partner(self):
        return (self.atom(flip=True), self.x)

    def beside(self, step):
        return (self.me, lax.rem(self.x + step + 4, 4))


def greet(devices):
    barrier = pltpu.get_barrier_semaphore()
    for device in devices:
        pl.semaphore_signal(barrier, inc=1, device_id=device, device_id_type=MESH)
    pl.semaphore_wait(barrier, len(devices))


class Wires:
    def __init__(self, send_sem, recv_sem, first=0):
        self.send_sem, self.recv_sem, self.first = send_sem, recv_sem, first

    def copy(self, src, dst, at, device):
        return pltpu.make_async_remote_copy(
            src_ref=src,
            dst_ref=dst,
            send_sem=self.send_sem,
            recv_sem=self.recv_sem.at[self.first + at],
            device_id=device,
            device_id_type=MESH,
        )

    def send(self, src, dst, at, device):
        self.copy(src, dst, at, device).start()

    def wait(self, view, at, device):
        self.copy(view, view, at, device).wait_recv()

    def drain(self, view, device):
        self.copy(view, view, 0, device).wait_send()


OFFSETS = (0, -1, 1, 2)
SLOTS = (0, 2, 1, 3)
AXES = (("z", "y"), ("y", "z"))


class Gather:
    BASE = 15
    TOTAL = 2 * BASE

    def __init__(self, place, wires, own, full, sub, group):
        self.place, self.wires, self.own = place, wires, own
        self.full, self.sub, self.group = full, sub, group

    def origin(self, h, k, m):
        first, second = AXES[h]
        return self.place.atom(**{first: OFFSETS[k], second: OFFSETS[m]})

    def chunk(self, h, k, m):
        return self.full(h, self.origin(h, k, m))

    def to(self, h, order, s):
        return self.place.along(AXES[h][order], 1 - 2 * s)

    def source(self, h, k, m):
        return self.own(h) if (k, m) == (0, 0) else self.chunk(h, k, m)

    def start(self, h, s):
        self.wires.send(self.own(h), self.chunk(h, 0, 0), self.BASE * h + s, self.to(h, 0, s))

    def relay(self, h, s):
        piece = self.sub(h, self.origin(h, s + 1, 0), s)
        self.wires.send(piece, piece, self.BASE * h + 2, self.to(h, 0, s))

    def spread(self, h, k, s):
        self.wires.send(
            self.source(h, k, 0), self.chunk(h, k, 0), self.BASE * h + 3 + 3 * k + s,
            self.to(h, 1, s),
        )

    def pass_on(self, h, k, s):
        piece = self.sub(h, self.origin(h, k, s + 1), s)
        self.wires.send(piece, piece, self.BASE * h + 5 + 3 * k, self.to(h, 1, s))

    def across(self, h, k, m):
        self.wires.send(
            self.source(h, k, m), self.chunk(h, k, m),
            self.TOTAL + self.group(h, k, m), self.place.partner(),
        )

    def arrived1(self, h, s):
        self.wires.wait(self.chunk(h, s + 1, 0), self.BASE * h + s, self.to(h, 0, s))

    def arrived1s(self, h):
        self.wires.wait(self.chunk(h, 3, 0), self.BASE * h + 2, self.to(h, 0, 0))

    def arrived2(self, h, k, s):
        self.wires.wait(
            self.chunk(h, k, s + 1), self.BASE * h + 3 + 3 * k + s, self.to(h, 1, s)
        )

    def arrived2s(self, h, k):
        self.wires.wait(self.chunk(h, k, 3), self.BASE * h + 5 + 3 * k, self.to(h, 1, 0))

    def from_partner(self, view, n):
        self.wires.wait(view, self.TOTAL + n, self.place.partner())


class RingSum:
    def __init__(self, place, wires, count, part, near, final):
        self.place, self.wires, self.count = place, wires, count
        self.part, self.near, self.final = part, near, final
        half = (count + 1) // 2
        self.cut = (pl.ds(0, half), pl.ds(half, count - half))
        self.size = (half, count - half)

    def klass(self, step):
        return lax.rem(self.place.x + step + 4, 4)

    def to(self, s):
        return self.place.beside(2 * s - 1)

    def near_at(self, s):
        return self.near.at[s, pl.ds(0, self.size[s])]

    def far(self, s):
        self.wires.send(self.part(self.klass(2), self.cut[s]), self.near_at(s), s, self.to(s))

    def plain(self, s):
        cut = self.cut[1 - s]
        self.wires.send(
            self.part(self.klass(2 * s - 1), cut), self.final.at[s, cut], 2, self.to(s)
        )

    def mixed(self, s):
        cut = self.cut[s]
        mine = self.part(self.klass(2 * s - 1), cut)
        mine[...] = mine[...] + self.near[s, 0 : self.size[s]]
        self.wires.send(mine, self.final.at[s, cut], 2, self.to(s))

    def arrived(self, s):
        self.wires.wait(self.near_at(s), s, self.to(s))

    def total(self):
        self.wires.wait(self.final, 2, self.to(0))
        own = self.part(self.place.x, pl.ds(0, self.count))
        return own[...] + (self.final[0] + self.final[1])


def kernel(
    blk_in, pao_size_in, cabs_size_in, pao, cabs, weight_in, out,
    blk, pao_size, cabs_size, blk_rows, weight, own, every, chosen, margins, parts, nears, finals, held, vals, vnear, vfinal,
    send_a, recv_a, send_b, recv_b, send_c, recv_c, send_v, recv_v, local,
):
    place = Place()
    x = place.x
    load = [
        pltpu.make_async_copy(pao, own.at[pl.ds(0, 48)], local.at[0]),
        pltpu.make_async_copy(cabs, own.at[pl.ds(48, 96)], local.at[1]),
    ] + [
        pltpu.make_async_copy(
            pao.at[:, pl.ds(1920 * h, 1920)], every.at[32 * h + place.me], local.at[2 + h]
        )
        for h in range(2)
    ]
    load += [
        pltpu.make_async_copy(src, dst, local.at[4 + n])
        for n, (src, dst) in enumerate(
            (
                (blk_in, blk),
                (pao_size_in, pao_size),
                (cabs_size_in, cabs_size),
                (blk_in, blk_rows),
                (weight_in, weight),
            )
        )
    ]
    for copy in load:
        copy.start()
    greet(
        [place.along(a, s) for a in ("y", "z") for s in (1, -1)]
        + [place.partner(), place.beside(1), place.beside(-1)]
    )
    load[0].wait()
    cuts = ((0, 1024), (1024, 896))
    first = Gather(
        place,
        Wires(send_a, recv_a),
        lambda h: own.at[pl.ds(0, 48), pl.ds(1920 * h, 1920)],
        lambda h, atom: every.at[32 * h + atom],
        lambda h, atom, s: every.at[32 * h + atom, :, pl.ds(*cuts[s])],
        lambda h, k, m: m if h == 0 else k,
    )
    sums, gathers = [], [first]
    for r, (_, top, count) in enumerate(PARTS):
        sums.append(
            RingSum(
                place,
                Wires(send_b.at[r], recv_b, 3 * r),
                count,
                lambda k, span, r=r: parts[r].at[k, span],
                nears[r],
                finals[r],
            )
        )
        half = (count + 1) // 2
        span = ((top, half), (top + half, count - half))
        pieces = [
            ((t, (n + 1) // 2), (t + (n + 1) // 2, n // 2)) for t, n in span
        ]

        def tiles(atom, start, n):
            return held.at[pl.ds(atom * HELD + start, n)]

        gathers.append(
            Gather(
                place,
                Wires(send_c.at[r], recv_c, 31 * r),
                lambda h, span=span: tiles(place.me, *span[h]),
                lambda h, atom, span=span: tiles(atom, *span[h]),
                lambda h, atom, s, pieces=pieces: tiles(atom, *pieces[h][s]),
                lambda h, k, m: 0,
            )
        )

    def roots():
        w = weight[...].astype(jnp.float32)
        spot = lax.broadcasted_iota(jnp.int32, (8, 48), 1) - 12 * x
        row = lax.broadcasted_iota(jnp.int32, (8, 48), 0)

        def column(b, shift, mask):
            at = jnp.logical_and(mask, spot == row + shift)
            return jnp.where(at, jnp.broadcast_to(w[b : b + 1], (8, 48)), 0.0)

        return [
            jnp.sqrt(jnp.sum(part_w, axis=1, keepdims=True))
            for part_w in (
                column(0, 0, row >= 0),
                column(1, 0, row >= 0),
                column(0, 8, row < 4) + column(1, 4, row >= 4),
            )
        ]

    nt = (((1,), (1,)), ((), ()))

    def line_products(i):
        line = lax.rem(place.y + OFFSETS[i] + 4, 4)
        g = None
        for h in range(2):
            rows = every[pl.ds(32 * h + line * 8, 8)].reshape(384, 1920)
            d = lax.dot_general(
                own[48:, 1920 * h : 1920 * (h + 1)], rows, nt,
                preferred_element_type=jnp.float32,
            )
            g = d if g is None else g + d
        r = [i in lines for lines, _, _ in PARTS].index(True)
        start = 9 * PARTS[r][0].index(i)
        for c in range(3):
            col = g[:, 128 * c : 128 * c + 128]
            for k in range(4):
                a, b = 12 * k, 48 + 12 * k
                parts[r][k, start + c] = col[a : a + 8]
                parts[r][k, start + 3 + c] = col[b : b + 8]
                parts[r][k, start + 6 + c] = jnp.concatenate(
                    [col[a + 8 : a + 12], col[b + 8 : b + 12]], axis=0
                )

    def pick_blocks(i):
        line = lax.rem(place.y + OFFSETS[i] + 4, 4)
        slot = SLOTS[i]
        names = blk_rows[...]
        for j in range(4):
            odd = []
            for n in range(2):
                hit = jnp.where(names == 2 * (line * 8 + 2 * j + n) + 1, 1, 0)
                hit = jnp.max(jnp.max(hit, axis=1, keepdims=True), axis=0, keepdims=True)
                odd.append(jnp.broadcast_to(hit, (24, 1920)) > 0)
            for h in range(2):
                got = []
                for n in range(2):
                    rows = every[32 * h + line * 8 + 2 * j + n].astype(jnp.float32)
                    got.append(jnp.where(odd[n], rows[24:], rows[:24]))
                at = 192 * slot + 48 * j
                chosen[h, at : at + 48] = jnp.concatenate(got, axis=0).astype(jnp.bfloat16)

    def margin_block(a, b):
        g = None
        for h in range(2):
            d = lax.dot_general(
                chosen[h, 128 * a : 128 * a + 128], chosen[h, 256 * b : 256 * b + 256], nt,
                preferred_element_type=jnp.float32,
            )
            g = d if g is None else g + d
        for t in range(16):
            for c in range(2):
                margins[(16 * a + t) * 6 + 2 * b + c] = g[
                    8 * t : 8 * t + 8, 128 * c : 128 * c + 128
                ]

    mine = place.me * HELD

    def keep_part(r, root):
        total = sums[r].total()
        lines, top, count = PARTS[r]
        for n in range(3 * len(lines)):
            held[pl.ds(mine + top + 3 * n, 3)] = total[3 * n : 3 * n + 3] * root[n % 3]

    def line_sem(i):
        return ("d", 0, i)

    def needs(op):
        name, g = op[0], op[1]
        if name in (LINE, PICK):
            return [line_sem(g)]
        if name == BLOCK:
            return []
        if name in (FAR, PLAIN):
            return []
        if name == MIXED:
            return [("near", g, op[2])]
        if name == KEEP:
            return []
        h = op[2]
        reach = lambda k: [] if k == 0 else [("1", g, h, k - 1)] if k < 3 else [("1s", g, h)]
        if name == START:
            return []
        if name == RELAY:
            return [("1", g, h, op[3])]
        if name == SPREAD:
            return reach(op[3])
        if name == PASS:
            return [("2", g, h, op[3], op[4])]
        k, m = op[3], op[4]
        return reach(k) if m == 0 else [("2", g, h, k, m - 1)] if m < 3 else [("2s", g, h, k)]

    def settle(sem):
        kind, g = sem[0], sem[1]
        if kind == "d":
            first.from_partner(every.at[pl.ds(0, 8)], sem[2])
        elif kind == "near":
            sums[g].arrived(sem[2])
        else:
            at = {"1": "arrived1", "1s": "arrived1s", "2": "arrived2", "2s": "arrived2s"}[kind]
            getattr(gathers[g], at)(*sem[2:])

    settled, loading, root = set(), load[1:], None
    for op in ORDER:
        for sem in needs(op):
            if sem not in settled:
                settle(sem)
                settled.add(sem)
        name, g = op[0], op[1]
        if name in (LINE, PICK) and loading:
            for copy in loading:
                copy.wait()
            loading, root = [], roots()
        if name == LINE:
            line_products(g)
        elif name == PICK:
            pick_blocks(g)
        elif name == BLOCK:
            margin_block(g, op[2])
        elif name == KEEP:
            keep_part(g, root)
        elif name in (FAR, PLAIN, MIXED):
            ring = sums[g]
            {FAR: ring.far, PLAIN: ring.plain, MIXED: ring.mixed}[name](op[2])
        else:
            net = gathers[g]
            {
                START: net.start,
                RELAY: net.relay,
                SPREAD: net.spread,
                PASS: net.pass_on,
                ACROSS: net.across,
            }[name](*op[2:])
    for r, (_, _, count) in enumerate(PARTS):
        gathers[r + 1].from_partner(held.at[pl.ds(0, 16 * count)], 0)

    lanes = lax.broadcasted_iota(jnp.int32, (8, 128), 1)
    subs = lax.broadcasted_iota(jnp.int32, (8, 128), 0)

    def half_of(n, bits):
        return lax.shift_right_logical(n, jnp.int32(bits))

    def one_pair(p):
        picks = [blk[l, p] for l in range(4)]
        base = [half_of(b, 1) * HELD for b in picks]
        par = [jnp.bitwise_and(b, 1) for b in picks]
        lines = [half_of(b, 4) for b in picks]
        seats = []
        for b, line in zip(picks, lines):
            away = jnp.bitwise_and(line - place.y, 3)
            slot = jnp.bitwise_xor(away, half_of(away, 1))
            seats.append(slot * 8 + jnp.bitwise_and(half_of(b, 1), 7))
        acc = [None] * 20
        for l in range(4):
            off = jnp.bitwise_and(picks[l], 15) * 24
            u = half_of(off, 7)
            rem = jnp.bitwise_and(off, 127)
            turn = jnp.bitwise_and(24 * l + 128 - rem, 127)
            whole = lanes >= rem
            here = jnp.logical_and(lanes >= 24 * l, lanes < 24 * l + 24)
            off = seats[l] * 24
            um = half_of(off, 7)
            rem = jnp.bitwise_and(off, 127)
            turn_m = jnp.bitwise_and(24 * l + 128 - rem, 127)
            whole_m = lanes >= rem

            def place_in(n, two, whole, turn):
                moved = pltpu.roll(jnp.where(whole, two[0], two[1]), turn, 1)
                old = jnp.zeros_like(moved) if acc[n] is None else acc[n]
                acc[n] = jnp.where(here, moved, old)

            for k in range(4):
                m = margins[pl.ds(seats[k] * 18 + um, 14)]
                for t in range(3):
                    place_in(3 * k + t, (m[6 * t], m[6 * t + 1]), whole_m, turn_m)
                away = jnp.bitwise_and(lines[l] - lines[k], 3)
                at = base[k] + jnp.bitwise_xor(away, half_of(away, 1)) * 9 + u
                c = held[pl.ds(at + par[k] * 3, 2)]
                place_in(12 + 2 * k, (c[0], c[1]), whole, turn)
                c = held[pl.ds(at + 6, 2)]
                place_in(13 + 2 * k, (c[0], c[1]), whole, turn)
        limit = cabs_size[p] - 12 * x
        for k in range(4):
            first = subs < limit - 48 * k
            low = 4 * par[k]
            second = jnp.logical_and(
                jnp.logical_and(subs >= low, subs < low + 4),
                subs < limit - 48 * k - 8 + low,
            )
            acc[12 + 2 * k] = jnp.where(first, acc[12 + 2 * k], 0.0)
            acc[13 + 2 * k] = jnp.where(second, acc[13 + 2 * k], 0.0)
        margin = jnp.concatenate(acc[:12], axis=0)
        c = jnp.concatenate(acc[12:], axis=0)
        hi = c.astype(jnp.bfloat16)
        lo = (c - hi.astype(jnp.float32)).astype(jnp.bfloat16)
        prod = lax.dot_general(
            jnp.concatenate([hi, lo, hi], axis=0),
            jnp.concatenate([hi, hi, lo], axis=0),
            (((0,), (0,)), ((), ())),
            preferred_element_type=jnp.float32,
        )
        return margin - prod[:96]

    left, right = place.beside(-1), place.beside(1)
    klass = sums[0].klass

    def copy_v(kind, q):
        e, o = 2 * q, 2 * q + 1
        src, dst, device, at = (
            lambda: (vals.at[klass(2) * 16 + e], vnear.at[2 * q], left, 3 * q),
            lambda: (vals.at[klass(2) * 16 + o], vnear.at[2 * q + 1], right, 3 * q + 1),
            lambda: (vals.at[klass(-1) * 16 + o], vfinal.at[o], left, 3 * q + 2),
            lambda: (vals.at[klass(1) * 16 + e], vfinal.at[16 + e], right, 3 * q + 2),
            lambda: (vals.at[klass(-1) * 16 + e], vfinal.at[e], left, 3 * q + 2),
            lambda: (vals.at[klass(1) * 16 + o], vfinal.at[16 + o], right, 3 * q + 2),
        )[kind]()
        return Wires(send_v, recv_v).copy(src, dst, at, device)

    def second_step(q):
        e, o = klass(-1) * 16 + 2 * q, klass(1) * 16 + 2 * q + 1
        copy_v(0, q).wait_recv()
        vals[e] = vals[e] + vnear[2 * q]
        copy_v(4, q).start()
        copy_v(1, q).wait_recv()
        vals[o] = vals[o] + vnear[2 * q + 1]
        copy_v(5, q).start()

    wide = lax.broadcasted_iota(jnp.int32, (96, 128), 1)

    def group(g):
        v = [one_pair(g * 4 + n) for n in range(4)]
        r1 = pltpu.roll(v[1], 96, 1)
        r2 = pltpu.roll(v[2], 64, 1)
        r3 = pltpu.roll(v[3], 32, 1)
        packed = (
            jnp.where(wide < 96, v[0], r1),
            jnp.where(wide < 64, r1, r2),
            jnp.where(wide < 32, r2, r3),
        )
        for c in range(3):
            for k in range(4):
                vals[k * 16 + g, :, 128 * c : 128 * c + 128] = packed[c][24 * k : 24 * k + 24]

    @pl.loop(0, 8)
    def _(q):
        group(2 * q)
        copy_v(0, q).start()
        copy_v(3, q).start()
        group(2 * q + 1)
        copy_v(1, q).start()
        copy_v(2, q).start()

        @pl.when(q >= 3)
        def _():
            second_step(q - 3)

    for q in range(8 - 3, 8):
        second_step(q)

    narrow = lax.broadcasted_iota(jnp.int32, (24, 128), 1)
    deep = lax.broadcasted_iota(jnp.int32, (24, 128), 0) + 24 * x

    @pl.loop(0, 8)
    def _(q):
        view = vfinal.at[pl.ds(0, 4)]
        Wires(send_v, recv_v).wait(view, 3 * q + 2, left)
        for half in range(2):
            g = 2 * q + half
            t = vals[x * 16 + g] + (vfinal[g] + vfinal[16 + g])
            t0, t1, t2 = t[:, :128], t[:, 128:256], t[:, 256:]
            v = (
                t0,
                jnp.where(narrow < 32, pltpu.roll(t0, 32, 1), pltpu.roll(t1, 32, 1)),
                jnp.where(narrow < 64, pltpu.roll(t1, 64, 1), pltpu.roll(t2, 64, 1)),
                pltpu.roll(t2, 96, 1),
            )
            for n in range(4):
                size = pao_size[g * 4 + n]
                keep = jnp.logical_and(deep < size, narrow < size)
                out[g * 4 + n] = jnp.where(keep, v[n], 0.0)[:, :96]

    first.wires.drain(every.at[pl.ds(0, 62)], left)
    for r, (_, _, count) in enumerate(PARTS):
        sums[r].wires.drain(held.at[pl.ds(0, 3 * count)], left)
        gathers[r + 1].wires.drain(held.at[pl.ds(0, 31 * count)], left)
    Wires(send_v, recv_v).drain(vals.at[pl.ds(0, 48)], left)


def fused(blk, pao_size, cabs_size, pao, cabs, weight):
    dma = pltpu.SemaphoreType.DMA
    vmem = pl.BlockSpec(memory_space=pltpu.VMEM)
    hbm = pl.BlockSpec(memory_space=pltpu.HBM)
    f32 = jnp.float32
    return pl.pallas_call(
        kernel,
        out_shape=jax.ShapeDtypeStruct((64, 24, 96), f32),
        in_specs=[hbm] * 6,
        out_specs=vmem,
        scratch_shapes=[
            pltpu.SMEM((4, 64), jnp.int32),
            pltpu.SMEM((64,), jnp.int32),
            pltpu.SMEM((64,), jnp.int32),
            pltpu.VMEM((4, 64), jnp.int32),
            pltpu.VMEM((2, 48), jnp.bfloat16),
            pltpu.VMEM((144, 3840), jnp.bfloat16),
            pltpu.VMEM((64, 48, 1920), jnp.bfloat16),
            pltpu.VMEM((2, 768, 1920), jnp.bfloat16),
            pltpu.VMEM((CHOSEN, 8, 128), f32),
            [pltpu.VMEM((4, n, 8, 128), f32) for _, _, n in PARTS],
            [pltpu.VMEM((2, (n + 1) // 2, 8, 128), f32) for _, _, n in PARTS],
            [pltpu.VMEM((2, n, 8, 128), f32) for _, _, n in PARTS],
            pltpu.VMEM((32 * HELD, 8, 128), f32),
            pltpu.VMEM((64, 24, 384), f32),
            pltpu.VMEM((16, 24, 384), f32),
            pltpu.VMEM((32, 24, 384), f32),
            dma,
            dma((Gather.TOTAL + 4,)),
            dma((len(PARTS),)),
            dma((3 * len(PARTS),)),
            dma((len(PARTS),)),
            dma((31 * len(PARTS),)),
            dma,
            dma((24,)),
            dma((9,)),
        ],
        compiler_params=pltpu.CompilerParams(
            collective_id=0, has_side_effects=True, vmem_limit_bytes=56 * 1024 * 1024
        ),
        name="fused",
    )(blk, pao_size, cabs_size, pao, cabs, weight)


def shards(pao_blocks, cabs_blocks, cabs_weight, pair_blocks, pao_size, cabs_size):
    return fused(
        pair_blocks.T,
        pao_size,
        cabs_size,
        pao_blocks.reshape(48, -1),
        cabs_blocks.reshape(96, -1),
        cabs_weight,
    )


def solution(mesh):
    placed = (
        P("atom", None, "aux"),
        P("atom", None, "aux"),
        P("atom", None),
        P("atom", None),
        P("atom"),
        P("atom"),
    )
    return jax.shard_map(
        shards, mesh=mesh, in_specs=placed, out_specs=P("atom", "aux", None), check_vma=False
    )
```

```python
import jax
import jax.numpy as jnp
from jax import lax
from jax.experimental import pallas as pl
from jax.experimental.pallas import tpu as pltpu
from jax.sharding import PartitionSpec as P

MESH = pl.DeviceIdType.MESH

PARTS = (((0, 2), 0, 18), ((1,), 18, 9), ((3,), 27, 9), )
HELD = 37
CHOSEN = 577

START, RELAY, SPREAD, PASS, ACROSS, LINE = range(6)
FAR, PLAIN, MIXED, KEEP, PICK, BLOCK = range(6, 12)

ORDER = (
    (START, 0, 0, 0), (START, 0, 0, 1), (START, 0, 1, 0), (START, 0, 1, 1),
    (ACROSS, 0, 1, 0, 0), (ACROSS, 0, 0, 0, 0), (SPREAD, 0, 1, 0, 0),
    (SPREAD, 0, 1, 0, 1), (SPREAD, 0, 0, 0, 0), (SPREAD, 0, 0, 0, 1),
    (ACROSS, 0, 1, 2, 0), (ACROSS, 0, 1, 1, 0), (ACROSS, 0, 0, 1, 0), (RELAY, 0, 0, 0),
    (RELAY, 0, 0, 1), (RELAY, 0, 1, 0), (RELAY, 0, 1, 1), (ACROSS, 0, 0, 2, 0),
    (SPREAD, 0, 1, 2, 0), (SPREAD, 0, 1, 2, 1), (SPREAD, 0, 0, 1, 0),
    (SPREAD, 0, 0, 2, 1), (ACROSS, 0, 1, 0, 1), (ACROSS, 0, 1, 0, 2),
    (ACROSS, 0, 0, 0, 2), (ACROSS, 0, 0, 0, 1), (ACROSS, 0, 1, 3, 0),
    (ACROSS, 0, 0, 3, 0), (PASS, 0, 1, 0, 0), (PASS, 0, 1, 0, 1), (PASS, 0, 0, 0, 0),
    (SPREAD, 0, 0, 3, 1), (SPREAD, 0, 1, 1, 0), (SPREAD, 0, 1, 1, 1),
    (SPREAD, 0, 0, 3, 0), (ACROSS, 0, 1, 2, 2), (ACROSS, 0, 0, 2, 2),
    (ACROSS, 0, 0, 1, 1), (SPREAD, 0, 0, 1, 1), (ACROSS, 0, 1, 2, 1),
    (ACROSS, 0, 1, 0, 3), (PASS, 0, 1, 2, 0), (PASS, 0, 1, 2, 1), (SPREAD, 0, 0, 2, 0),
    (ACROSS, 0, 0, 3, 2), (LINE, 0), (SPREAD, 0, 1, 3, 0), (SPREAD, 0, 1, 3, 1),
    (PASS, 0, 0, 0, 1), (PICK, 0), (ACROSS, 0, 1, 1, 1), (ACROSS, 0, 1, 1, 2),
    (ACROSS, 0, 0, 3, 1), (PASS, 0, 0, 1, 0), (PASS, 0, 0, 3, 1), (ACROSS, 0, 1, 2, 3),
    (ACROSS, 0, 0, 1, 2), (PASS, 0, 1, 1, 0), (PASS, 0, 1, 1, 1), (PASS, 0, 0, 3, 0),
    (PASS, 0, 0, 1, 1), (ACROSS, 0, 0, 0, 3), (LINE, 2), (ACROSS, 0, 0, 2, 1),
    (PLAIN, 0, 1), (FAR, 0, 0), (PASS, 0, 0, 2, 0), (PASS, 0, 0, 2, 1), (PICK, 2),
    (PASS, 0, 1, 3, 0), (PASS, 0, 1, 3, 1), (ACROSS, 0, 1, 3, 2), (FAR, 0, 1),
    (PLAIN, 0, 0), (ACROSS, 0, 1, 3, 1), (ACROSS, 0, 1, 1, 3), (MIXED, 0, 0),
    (ACROSS, 0, 0, 3, 3), (MIXED, 0, 1), (ACROSS, 0, 0, 1, 3), (LINE, 1),
    (ACROSS, 0, 0, 2, 3), (FAR, 1, 1), (FAR, 1, 0), (ACROSS, 0, 1, 3, 3),
    (PLAIN, 1, 1), (PLAIN, 1, 0), (PICK, 1), (BLOCK, 0, 0), (BLOCK, 0, 1),
    (KEEP, 0), (SPREAD, 1, 1, 0, 0), (START, 1, 0, 1), (START, 1, 1, 0),
    (START, 1, 1, 1), (ACROSS, 1, 0, 0, 0), (LINE, 3), (ACROSS, 1, 1, 0, 0),
    (FAR, 2, 1), (FAR, 2, 0), (START, 1, 0, 0), (SPREAD, 1, 1, 0, 1),
    (SPREAD, 1, 0, 0, 0), (SPREAD, 1, 0, 0, 1), (PLAIN, 2, 1), (MIXED, 1, 0),
    (MIXED, 1, 1), (PLAIN, 2, 0), (PICK, 3), (BLOCK, 1, 0), (BLOCK, 1, 1),
    (SPREAD, 1, 1, 2, 0), (RELAY, 1, 0, 1), (RELAY, 1, 1, 0), (RELAY, 1, 1, 1),
    (ACROSS, 1, 1, 1, 0), (ACROSS, 1, 1, 2, 0), (ACROSS, 1, 1, 0, 1),
    (ACROSS, 1, 0, 2, 0), (MIXED, 2, 1), (MIXED, 2, 0), (SPREAD, 1, 1, 1, 1),
    (SPREAD, 1, 0, 2, 0), (SPREAD, 1, 0, 2, 1), (RELAY, 1, 0, 0), (ACROSS, 1, 0, 1, 0),
    (ACROSS, 1, 0, 0, 2), (ACROSS, 1, 1, 0, 2), (ACROSS, 1, 0, 0, 1), (KEEP, 1),
    (SPREAD, 1, 1, 1, 0), (SPREAD, 1, 1, 2, 1), (SPREAD, 1, 0, 1, 0),
    (SPREAD, 1, 0, 1, 1), (ACROSS, 2, 0, 0, 0), (ACROSS, 2, 1, 0, 0), (START, 2, 0, 0),
    (START, 2, 0, 1), (START, 2, 1, 0), (START, 2, 1, 1), (SPREAD, 2, 0, 0, 0),
    (SPREAD, 2, 0, 0, 1), (SPREAD, 2, 1, 0, 0), (SPREAD, 2, 1, 0, 1), (BLOCK, 2, 0),
    (BLOCK, 2, 1), (ACROSS, 1, 1, 3, 0), (SPREAD, 1, 1, 3, 0), (SPREAD, 1, 1, 3, 1),
    (PASS, 1, 0, 0, 0), (PASS, 1, 0, 0, 1), (KEEP, 2), (ACROSS, 1, 1, 2, 1),
    (START, 3, 1, 0), (START, 3, 1, 1), (ACROSS, 3, 0, 0, 0), (ACROSS, 3, 1, 0, 0),
    (ACROSS, 1, 1, 1, 2), (START, 3, 0, 0), (START, 3, 0, 1), (SPREAD, 1, 0, 3, 0),
    (SPREAD, 1, 0, 3, 1), (ACROSS, 1, 0, 3, 0), (ACROSS, 1, 0, 2, 1),
    (ACROSS, 1, 0, 2, 2), (SPREAD, 3, 1, 0, 0), (SPREAD, 3, 1, 0, 1), (BLOCK, 3, 0),
    (ACROSS, 1, 0, 1, 1), (PASS, 1, 1, 1, 0), (PASS, 1, 1, 2, 1), (SPREAD, 3, 0, 0, 0),
    (SPREAD, 3, 0, 0, 1), (ACROSS, 1, 0, 1, 2), (ACROSS, 1, 1, 2, 2),
    (ACROSS, 2, 1, 1, 0), (ACROSS, 2, 1, 2, 0), (RELAY, 2, 0, 0), (RELAY, 2, 0, 1),
    (ACROSS, 2, 0, 2, 0), (RELAY, 2, 1, 0), (RELAY, 2, 1, 1), (ACROSS, 2, 0, 1, 0),
    (ACROSS, 1, 1, 1, 1), (SPREAD, 2, 1, 1, 0), (SPREAD, 2, 1, 2, 1),
    (SPREAD, 2, 0, 2, 0), (SPREAD, 2, 0, 1, 1), (ACROSS, 2, 0, 0, 1),
    (ACROSS, 2, 0, 0, 2), (ACROSS, 2, 1, 0, 1), (ACROSS, 2, 1, 0, 2),
    (SPREAD, 2, 1, 2, 0), (SPREAD, 2, 1, 1, 1), (SPREAD, 2, 0, 1, 0),
    (SPREAD, 2, 0, 2, 1), (BLOCK, 3, 1), (ACROSS, 1, 0, 0, 3), (PASS, 1, 1, 0, 0),
    (PASS, 1, 1, 1, 1), (ACROSS, 1, 1, 3, 1), (PASS, 1, 0, 1, 0), (PASS, 1, 0, 2, 1),
    (ACROSS, 1, 1, 3, 2), (SPREAD, 3, 1, 1, 0), (SPREAD, 3, 1, 1, 1),
    (ACROSS, 3, 1, 2, 0), (ACROSS, 3, 1, 1, 0), (RELAY, 3, 1, 0), (RELAY, 3, 1, 1),
    (ACROSS, 3, 0, 1, 0), (ACROSS, 3, 0, 2, 0), (RELAY, 3, 0, 0), (RELAY, 3, 0, 1),
    (SPREAD, 3, 0, 1, 0), (SPREAD, 3, 0, 1, 1), (SPREAD, 3, 1, 2, 0),
    (SPREAD, 3, 1, 2, 1), (ACROSS, 3, 1, 0, 1), (ACROSS, 1, 0, 3, 1),
    (ACROSS, 1, 0, 3, 2), (SPREAD, 3, 0, 2, 0), (SPREAD, 3, 0, 2, 1),
    (ACROSS, 3, 1, 0, 2), (PASS, 3, 1, 0, 0), (PASS, 3, 1, 0, 1), (BLOCK, 0, 2),
    (ACROSS, 3, 0, 0, 1), (PASS, 1, 1, 3, 0), (PASS, 1, 1, 0, 1), (ACROSS, 3, 0, 0, 2),
    (ACROSS, 2, 0, 3, 0), (PASS, 3, 0, 0, 0), (PASS, 3, 0, 0, 1), (ACROSS, 2, 1, 3, 0),
    (SPREAD, 2, 0, 3, 0), (SPREAD, 2, 0, 3, 1), (SPREAD, 2, 1, 3, 0),
    (SPREAD, 2, 1, 3, 1), (ACROSS, 2, 1, 2, 2), (ACROSS, 2, 1, 1, 1),
    (ACROSS, 2, 0, 2, 1), (ACROSS, 2, 0, 1, 2), (PASS, 1, 1, 2, 0), (PASS, 1, 1, 3, 1),
    (ACROSS, 2, 1, 2, 1), (PASS, 1, 0, 3, 0), (PASS, 1, 0, 3, 1), (ACROSS, 2, 1, 1, 2),
    (ACROSS, 2, 0, 1, 1), (ACROSS, 2, 0, 2, 2), (PASS, 2, 1, 1, 0), (PASS, 2, 1, 1, 1),
    (BLOCK, 1, 2), (ACROSS, 1, 1, 1, 3), (PASS, 1, 0, 2, 0), (PASS, 1, 0, 1, 1),
    (PASS, 2, 1, 2, 0), (PASS, 2, 1, 2, 1), (PASS, 2, 1, 0, 0), (PASS, 2, 1, 0, 1),
    (ACROSS, 3, 1, 1, 1), (ACROSS, 3, 1, 3, 0), (PASS, 2, 0, 0, 0), (PASS, 2, 0, 0, 1),
    (ACROSS, 3, 1, 1, 2), (PASS, 3, 1, 1, 0), (PASS, 3, 1, 1, 1), (ACROSS, 3, 0, 3, 0),
    (SPREAD, 3, 0, 3, 0), (SPREAD, 3, 0, 3, 1), (SPREAD, 3, 1, 3, 0),
    (SPREAD, 3, 1, 3, 1), (ACROSS, 3, 0, 1, 2), (ACROSS, 3, 0, 1, 1),
    (ACROSS, 3, 1, 2, 1), (PASS, 3, 1, 2, 0), (PASS, 3, 1, 2, 1), (ACROSS, 3, 1, 2, 2),
    (PASS, 3, 0, 1, 0), (PASS, 3, 0, 1, 1), (ACROSS, 3, 1, 0, 3), (ACROSS, 3, 0, 2, 1),
    (PASS, 3, 0, 2, 0), (PASS, 3, 0, 2, 1), (ACROSS, 3, 0, 2, 2), (BLOCK, 2, 2),
    (ACROSS, 3, 0, 0, 3), (PASS, 2, 0, 2, 0), (PASS, 2, 0, 1, 1), (ACROSS, 1, 1, 0, 3),
    (PASS, 2, 0, 1, 0), (PASS, 2, 0, 2, 1), (PASS, 2, 1, 3, 0), (PASS, 2, 1, 3, 1),
    (ACROSS, 2, 1, 3, 1), (ACROSS, 2, 1, 3, 2), (PASS, 2, 0, 3, 0), (PASS, 2, 0, 3, 1),
    (ACROSS, 2, 0, 3, 2), (ACROSS, 2, 0, 3, 1), (ACROSS, 1, 1, 2, 3),
    (ACROSS, 1, 0, 3, 3), (ACROSS, 1, 1, 3, 3), (BLOCK, 3, 2), (ACROSS, 2, 1, 2, 3),
    (ACROSS, 2, 1, 1, 3), (ACROSS, 1, 0, 1, 3), (ACROSS, 1, 0, 2, 3),
    (ACROSS, 2, 0, 0, 3), (ACROSS, 3, 1, 1, 3), (ACROSS, 2, 1, 0, 3), (BLOCK, 4, 0),
    (PASS, 3, 1, 3, 0), (PASS, 3, 1, 3, 1), (ACROSS, 3, 1, 3, 1), (ACROSS, 3, 1, 3, 2),
    (PASS, 3, 0, 3, 0), (PASS, 3, 0, 3, 1), (ACROSS, 3, 0, 3, 1), (ACROSS, 3, 0, 3, 2),
    (ACROSS, 3, 1, 2, 3), (ACROSS, 3, 0, 1, 3), (ACROSS, 3, 0, 2, 3), (BLOCK, 4, 1),
    (ACROSS, 2, 0, 2, 3), (ACROSS, 2, 0, 1, 3), (ACROSS, 2, 1, 3, 3),
    (ACROSS, 2, 0, 3, 3), (BLOCK, 4, 2), (BLOCK, 5, 0), (ACROSS, 3, 1, 3, 3),
    (ACROSS, 3, 0, 3, 3), (BLOCK, 5, 1), (BLOCK, 5, 2),
)


class Place:
    def __init__(self):
        self.me = lax.axis_index("atom")
        self.x = lax.axis_index("aux")
        self.core = lax.rem(self.me, 2)
        self.z = lax.rem(self.me // 2, 4)
        self.y = self.me // 8

    def atom(self, y=0, z=0, flip=False):
        core = 1 - self.core if flip else self.core
        return (lax.rem(self.y + y + 4, 4) * 4 + lax.rem(self.z + z + 4, 4)) * 2 + core

    def along(self, axis, step):
        at = self.atom(**{axis: step})
        return (at, self.x)

    def partner(self):
        return (self.atom(flip=True), self.x)

    def beside(self, step):
        return (self.me, lax.rem(self.x + step + 4, 4))


def greet(devices):
    barrier = pltpu.get_barrier_semaphore()
    for device in devices:
        pl.semaphore_signal(barrier, inc=1, device_id=device, device_id_type=MESH)
    pl.semaphore_wait(barrier, len(devices))


class Wires:
    def __init__(self, send_sem, recv_sem, first=0):
        self.send_sem, self.recv_sem, self.first = send_sem, recv_sem, first

    def copy(self, src, dst, at, device):
        return pltpu.make_async_remote_copy(
            src_ref=src,
            dst_ref=dst,
            send_sem=self.send_sem,
            recv_sem=self.recv_sem.at[self.first + at],
            device_id=device,
            device_id_type=MESH,
        )

    def send(self, src, dst, at, device):
        self.copy(src, dst, at, device).start()

    def wait(self, view, at, device):
        self.copy(view, view, at, device).wait_recv()

    def drain(self, view, device):
        self.copy(view, view, 0, device).wait_send()


OFFSETS = (0, -1, 1, 2)
SLOTS = (0, 2, 1, 3)
AXES = (("z", "y"), ("y", "z"))


class Gather:
    BASE = 15
    TOTAL = 2 * BASE

    def __init__(self, place, wires, own, full, sub, group):
        self.place, self.wires, self.own = place, wires, own
        self.full, self.sub, self.group = full, sub, group

    def origin(self, h, k, m):
        first, second = AXES[h]
        return self.place.atom(**{first: OFFSETS[k], second: OFFSETS[m]})

    def chunk(self, h, k, m):
        return self.full(h, self.origin(h, k, m))

    def to(self, h, order, s):
        return self.place.along(AXES[h][order], 1 - 2 * s)

    def source(self, h, k, m):
        return self.own(h) if (k, m) == (0, 0) else self.chunk(h, k, m)

    def start(self, h, s):
        self.wires.send(self.own(h), self.chunk(h, 0, 0), self.BASE * h + s, self.to(h, 0, s))

    def relay(self, h, s):
        piece = self.sub(h, self.origin(h, s + 1, 0), s)
        self.wires.send(piece, piece, self.BASE * h + 2, self.to(h, 0, s))

    def spread(self, h, k, s):
        self.wires.send(
            self.source(h, k, 0), self.chunk(h, k, 0), self.BASE * h + 3 + 3 * k + s,
            self.to(h, 1, s),
        )

    def pass_on(self, h, k, s):
        piece = self.sub(h, self.origin(h, k, s + 1), s)
        self.wires.send(piece, piece, self.BASE * h + 5 + 3 * k, self.to(h, 1, s))

    def across(self, h, k, m):
        self.wires.send(
            self.source(h, k, m), self.chunk(h, k, m),
            self.TOTAL + self.group(h, k, m), self.place.partner(),
        )

    def arrived1(self, h, s):
        self.wires.wait(self.chunk(h, s + 1, 0), self.BASE * h + s, self.to(h, 0, s))

    def arrived1s(self, h):
        self.wires.wait(self.chunk(h, 3, 0), self.BASE * h + 2, self.to(h, 0, 0))

    def arrived2(self, h, k, s):
        self.wires.wait(
            self.chunk(h, k, s + 1), self.BASE * h + 3 + 3 * k + s, self.to(h, 1, s)
        )

    def arrived2s(self, h, k):
        self.wires.wait(self.chunk(h, k, 3), self.BASE * h + 5 + 3 * k, self.to(h, 1, 0))

    def from_partner(self, view, n):
        self.wires.wait(view, self.TOTAL + n, self.place.partner())


class RingSum:
    def __init__(self, place, wires, count, part, near, final):
        self.place, self.wires, self.count = place, wires, count
        self.part, self.near, self.final = part, near, final
        half = (count + 1) // 2
        self.cut = (pl.ds(0, half), pl.ds(half, count - half))
        self.size = (half, count - half)

    def klass(self, step):
        return lax.rem(self.place.x + step + 4, 4)

    def to(self, s):
        return self.place.beside(2 * s - 1)

    def near_at(self, s):
        return self.near.at[s, pl.ds(0, self.size[s])]

    def far(self, s):
        self.wires.send(self.part(self.klass(2), self.cut[s]), self.near_at(s), s, self.to(s))

    def plain(self, s):
        cut = self.cut[1 - s]
        self.wires.send(
            self.part(self.klass(2 * s - 1), cut), self.final.at[s, cut], 2, self.to(s)
        )

    def mixed(self, s):
        cut = self.cut[s]
        mine = self.part(self.klass(2 * s - 1), cut)
        mine[...] = mine[...] + self.near[s, 0 : self.size[s]]
        self.wires.send(mine, self.final.at[s, cut], 2, self.to(s))

    def arrived(self, s):
        self.wires.wait(self.near_at(s), s, self.to(s))

    def total(self):
        self.wires.wait(self.final, 2, self.to(0))
        own = self.part(self.place.x, pl.ds(0, self.count))
        return own[...] + (self.final[0] + self.final[1])


def kernel(
    blk_in, pao_size_in, cabs_size_in, pao, cabs, weight_in, out,
    blk, pao_size, cabs_size, blk_rows, weight, own, every, chosen, margins, parts, nears, finals, held, vals, vnear, vfinal,
    send_a, recv_a, send_b, recv_b, send_c, recv_c, send_v, recv_v, local,
):
    place = Place()
    x = place.x
    load = [
        pltpu.make_async_copy(pao, own.at[pl.ds(0, 48)], local.at[0]),
        pltpu.make_async_copy(cabs, own.at[pl.ds(48, 96)], local.at[1]),
    ] + [
        pltpu.make_async_copy(
            pao.at[:, pl.ds(1920 * h, 1920)], every.at[32 * h + place.me], local.at[2 + h]
        )
        for h in range(2)
    ]
    load += [
        pltpu.make_async_copy(src, dst, local.at[4 + n])
        for n, (src, dst) in enumerate(
            (
                (blk_in, blk),
                (pao_size_in, pao_size),
                (cabs_size_in, cabs_size),
                (blk_in, blk_rows),
                (weight_in, weight),
            )
        )
    ]
    for copy in load:
        copy.start()
    greet(
        [place.along(a, s) for a in ("y", "z") for s in (1, -1)]
        + [place.partner(), place.beside(1), place.beside(-1)]
    )
    load[0].wait()
    cuts = ((0, 1024), (1024, 896))
    first = Gather(
        place,
        Wires(send_a, recv_a),
        lambda h: own.at[pl.ds(0, 48), pl.ds(1920 * h, 1920)],
        lambda h, atom: every.at[32 * h + atom],
        lambda h, atom, s: every.at[32 * h + atom, :, pl.ds(*cuts[s])],
        lambda h, k, m: m if h == 0 else k,
    )
    sums, gathers = [], [first]
    for r, (_, top, count) in enumerate(PARTS):
        sums.append(
            RingSum(
                place,
                Wires(send_b.at[r], recv_b, 3 * r),
                count,
                lambda k, span, r=r: parts[r].at[k, span],
                nears[r],
                finals[r],
            )
        )
        half = (count + 1) // 2
        span = ((top, half), (top + half, count - half))
        pieces = [
            ((t, (n + 1) // 2), (t + (n + 1) // 2, n // 2)) for t, n in span
        ]

        def tiles(atom, start, n):
            return held.at[pl.ds(atom * HELD + start, n)]

        gathers.append(
            Gather(
                place,
                Wires(send_c.at[r], recv_c, 31 * r),
                lambda h, span=span: tiles(place.me, *span[h]),
                lambda h, atom, span=span: tiles(atom, *span[h]),
                lambda h, atom, s, pieces=pieces: tiles(atom, *pieces[h][s]),
                lambda h, k, m: 0,
            )
        )

    def roots():
        w = weight[...].astype(jnp.float32)
        spot = lax.broadcasted_iota(jnp.int32, (8, 48), 1) - 12 * x
        row = lax.broadcasted_iota(jnp.int32, (8, 48), 0)

        def column(b, shift, mask):
            at = jnp.logical_and(mask, spot == row + shift)
            return jnp.where(at, jnp.broadcast_to(w[b : b + 1], (8, 48)), 0.0)

        return [
            jnp.sqrt(jnp.sum(part_w, axis=1, keepdims=True))
            for part_w in (
                column(0, 0, row >= 0),
                column(1, 0, row >= 0),
                column(0, 8, row < 4) + column(1, 4, row >= 4),
            )
        ]

    nt = (((1,), (1,)), ((), ()))

    def line_products(i):
        line = lax.rem(place.y + OFFSETS[i] + 4, 4)
        g = None
        for h in range(2):
            rows = every[pl.ds(32 * h + line * 8, 8)].reshape(384, 1920)
            d = lax.dot_general(
                own[48:, 1920 * h : 1920 * (h + 1)], rows, nt,
                preferred_element_type=jnp.float32,
            )
            g = d if g is None else g + d
        r = [i in lines for lines, _, _ in PARTS].index(True)
        start = 9 * PARTS[r][0].index(i)
        for c in range(3):
            col = g[:, 128 * c : 128 * c + 128]
            for k in range(4):
                a, b = 12 * k, 48 + 12 * k
                parts[r][k, start + c] = col[a : a + 8]
                parts[r][k, start + 3 + c] = col[b : b + 8]
                parts[r][k, start + 6 + c] = jnp.concatenate(
                    [col[a + 8 : a + 12], col[b + 8 : b + 12]], axis=0
                )

    def pick_blocks(i):
        line = lax.rem(place.y + OFFSETS[i] + 4, 4)
        slot = SLOTS[i]
        names = blk_rows[...]
        for j in range(4):
            odd = []
            for n in range(2):
                hit = jnp.where(names == 2 * (line * 8 + 2 * j + n) + 1, 1, 0)
                hit = jnp.max(jnp.max(hit, axis=1, keepdims=True), axis=0, keepdims=True)
                odd.append(jnp.broadcast_to(hit, (24, 1920)) > 0)
            for h in range(2):
                got = []
                for n in range(2):
                    rows = every[32 * h + line * 8 + 2 * j + n].astype(jnp.float32)
                    got.append(jnp.where(odd[n], rows[24:], rows[:24]))
                at = 192 * slot + 48 * j
                chosen[h, at : at + 48] = jnp.concatenate(got, axis=0).astype(jnp.bfloat16)

    def margin_block(a, b):
        g = None
        for h in range(2):
            d = lax.dot_general(
                chosen[h, 128 * a : 128 * a + 128], chosen[h, 256 * b : 256 * b + 256], nt,
                preferred_element_type=jnp.float32,
            )
            g = d if g is None else g + d
        for t in range(16):
            for c in range(2):
                margins[(16 * a + t) * 6 + 2 * b + c] = g[
                    8 * t : 8 * t + 8, 128 * c : 128 * c + 128
                ]

    mine = place.me * HELD

    def keep_part(r, root):
        total = sums[r].total()
        lines, top, count = PARTS[r]
        for n in range(3 * len(lines)):
            held[pl.ds(mine + top + 3 * n, 3)] = total[3 * n : 3 * n + 3] * root[n % 3]

    def line_sem(i):
        return ("d", 0, i)

    def needs(op):
        name, g = op[0], op[1]
        if name in (LINE, PICK):
            return [line_sem(g)]
        if name == BLOCK:
            return []
        if name in (FAR, PLAIN):
            return []
        if name == MIXED:
            return [("near", g, op[2])]
        if name == KEEP:
            return []
        h = op[2]
        reach = lambda k: [] if k == 0 else [("1", g, h, k - 1)] if k < 3 else [("1s", g, h)]
        if name == START:
            return []
        if name == RELAY:
            return [("1", g, h, op[3])]
        if name == SPREAD:
            return reach(op[3])
        if name == PASS:
            return [("2", g, h, op[3], op[4])]
        k, m = op[3], op[4]
        return reach(k) if m == 0 else [("2", g, h, k, m - 1)] if m < 3 else [("2s", g, h, k)]

    def settle(sem):
        kind, g = sem[0], sem[1]
        if kind == "d":
            first.from_partner(every.at[pl.ds(0, 8)], sem[2])
        elif kind == "near":
            sums[g].arrived(sem[2])
        else:
            at = {"1": "arrived1", "1s": "arrived1s", "2": "arrived2", "2s": "arrived2s"}[kind]
            getattr(gathers[g], at)(*sem[2:])

    settled, loading, root = set(), load[1:], None
    for op in ORDER:
        for sem in needs(op):
            if sem not in settled:
                settle(sem)
                settled.add(sem)
        name, g = op[0], op[1]
        if name in (LINE, PICK) and loading:
            for copy in loading:
                copy.wait()
            loading, root = [], roots()
        if name == LINE:
            line_products(g)
        elif name == PICK:
            pick_blocks(g)
        elif name == BLOCK:
            margin_block(g, op[2])
        elif name == KEEP:
            keep_part(g, root)
        elif name in (FAR, PLAIN, MIXED):
            ring = sums[g]
            {FAR: ring.far, PLAIN: ring.plain, MIXED: ring.mixed}[name](op[2])
        else:
            net = gathers[g]
            {
                START: net.start,
                RELAY: net.relay,
                SPREAD: net.spread,
                PASS: net.pass_on,
                ACROSS: net.across,
            }[name](*op[2:])
    for r, (_, _, count) in enumerate(PARTS):
        gathers[r + 1].from_partner(held.at[pl.ds(0, 16 * count)], 0)

    lanes = lax.broadcasted_iota(jnp.int32, (8, 128), 1)
    subs = lax.broadcasted_iota(jnp.int32, (8, 128), 0)

    def half_of(n, bits):
        return lax.shift_right_logical(n, jnp.int32(bits))

    def one_pair(p):
        picks = [blk[l, p] for l in range(4)]
        base = [half_of(b, 1) * HELD for b in picks]
        par = [jnp.bitwise_and(b, 1) for b in picks]
        lines = [half_of(b, 4) for b in picks]
        seats = []
        for b, line in zip(picks, lines):
            away = jnp.bitwise_and(line - place.y, 3)
            slot = jnp.bitwise_xor(away, half_of(away, 1))
            seats.append(slot * 8 + jnp.bitwise_and(half_of(b, 1), 7))
        acc = [None] * 20
        for l in range(4):
            off = jnp.bitwise_and(picks[l], 15) * 24
            u = half_of(off, 7)
            rem = jnp.bitwise_and(off, 127)
            turn = jnp.bitwise_and(24 * l + 128 - rem, 127)
            whole = lanes >= rem
            here = jnp.logical_and(lanes >= 24 * l, lanes < 24 * l + 24)
            off = seats[l] * 24
            um = half_of(off, 7)
            rem = jnp.bitwise_and(off, 127)
            turn_m = jnp.bitwise_and(24 * l + 128 - rem, 127)
            whole_m = lanes >= rem

            def place_in(n, two, whole, turn):
                moved = pltpu.roll(jnp.where(whole, two[0], two[1]), turn, 1)
                old = jnp.zeros_like(moved) if acc[n] is None else acc[n]
                acc[n] = jnp.where(here, moved, old)

            for k in range(4):
                m = margins[pl.ds(seats[k] * 18 + um, 14)]
                for t in range(3):
                    place_in(3 * k + t, (m[6 * t], m[6 * t + 1]), whole_m, turn_m)
                away = jnp.bitwise_and(lines[l] - lines[k], 3)
                at = base[k] + jnp.bitwise_xor(away, half_of(away, 1)) * 9 + u
                c = held[pl.ds(at + par[k] * 3, 2)]
                place_in(12 + 2 * k, (c[0], c[1]), whole, turn)
                c = held[pl.ds(at + 6, 2)]
                place_in(13 + 2 * k, (c[0], c[1]), whole, turn)
        limit = cabs_size[p] - 12 * x
        for k in range(4):
            first = subs < limit - 48 * k
            low = 4 * par[k]
            second = jnp.logical_and(
                jnp.logical_and(subs >= low, subs < low + 4),
                subs < limit - 48 * k - 8 + low,
            )
            acc[12 + 2 * k] = jnp.where(first, acc[12 + 2 * k], 0.0)
            acc[13 + 2 * k] = jnp.where(second, acc[13 + 2 * k], 0.0)
        margin = jnp.concatenate(acc[:12], axis=0)
        c = jnp.concatenate(acc[12:], axis=0)
        hi = c.astype(jnp.bfloat16)
        lo = (c - hi.astype(jnp.float32)).astype(jnp.bfloat16)
        prod = lax.dot_general(
            jnp.concatenate([hi, lo, hi], axis=0),
            jnp.concatenate([hi, hi, lo], axis=0),
            (((0,), (0,)), ((), ())),
            preferred_element_type=jnp.float32,
        )
        return margin - prod[:96]

    left, right = place.beside(-1), place.beside(1)
    klass = sums[0].klass

    def copy_v(kind, q):
        e, o = 2 * q, 2 * q + 1
        src, dst, device, at = (
            lambda: (vals.at[klass(2) * 16 + e], vnear.at[2 * q], left, 3 * q),
            lambda: (vals.at[klass(2) * 16 + o], vnear.at[2 * q + 1], right, 3 * q + 1),
            lambda: (vals.at[klass(-1) * 16 + o], vfinal.at[o], left, 3 * q + 2),
            lambda: (vals.at[klass(1) * 16 + e], vfinal.at[16 + e], right, 3 * q + 2),
            lambda: (vals.at[klass(-1) * 16 + e], vfinal.at[e], left, 3 * q + 2),
            lambda: (vals.at[klass(1) * 16 + o], vfinal.at[16 + o], right, 3 * q + 2),
        )[kind]()
        return Wires(send_v, recv_v).copy(src, dst, at, device)

    def second_step(q):
        e, o = klass(-1) * 16 + 2 * q, klass(1) * 16 + 2 * q + 1
        copy_v(0, q).wait_recv()
        vals[e] = vals[e] + vnear[2 * q]
        copy_v(4, q).start()
        copy_v(1, q).wait_recv()
        vals[o] = vals[o] + vnear[2 * q + 1]
        copy_v(5, q).start()

    wide = lax.broadcasted_iota(jnp.int32, (96, 128), 1)

    def group(g):
        v = [one_pair(g * 4 + n) for n in range(4)]
        r1 = pltpu.roll(v[1], 96, 1)
        r2 = pltpu.roll(v[2], 64, 1)
        r3 = pltpu.roll(v[3], 32, 1)
        packed = (
            jnp.where(wide < 96, v[0], r1),
            jnp.where(wide < 64, r1, r2),
            jnp.where(wide < 32, r2, r3),
        )
        for c in range(3):
            for k in range(4):
                vals[k * 16 + g, :, 128 * c : 128 * c + 128] = packed[c][24 * k : 24 * k + 24]

    @pl.loop(0, 8)
    def _(q):
        group(2 * q)
        copy_v(0, q).start()
        copy_v(3, q).start()
        group(2 * q + 1)
        copy_v(1, q).start()
        copy_v(2, q).start()

        @pl.when(q >= 4)
        def _():
            second_step(q - 4)

    for q in range(4, 8):
        second_step(q)

    narrow = lax.broadcasted_iota(jnp.int32, (24, 128), 1)
    deep = lax.broadcasted_iota(jnp.int32, (24, 128), 0) + 24 * x

    @pl.loop(0, 8)
    def _(q):
        view = vfinal.at[pl.ds(0, 4)]
        Wires(send_v, recv_v).wait(view, 3 * q + 2, left)
        for half in range(2):
            g = 2 * q + half
            t = vals[x * 16 + g] + (vfinal[g] + vfinal[16 + g])
            t0, t1, t2 = t[:, :128], t[:, 128:256], t[:, 256:]
            v = (
                t0,
                jnp.where(narrow < 32, pltpu.roll(t0, 32, 1), pltpu.roll(t1, 32, 1)),
                jnp.where(narrow < 64, pltpu.roll(t1, 64, 1), pltpu.roll(t2, 64, 1)),
                pltpu.roll(t2, 96, 1),
            )
            for n in range(4):
                size = pao_size[g * 4 + n]
                keep = jnp.logical_and(deep < size, narrow < size)
                out[g * 4 + n] = jnp.where(keep, v[n], 0.0)[:, :96]

    first.wires.drain(every.at[pl.ds(0, 62)], left)
    for r, (_, _, count) in enumerate(PARTS):
        sums[r].wires.drain(held.at[pl.ds(0, 3 * count)], left)
        gathers[r + 1].wires.drain(held.at[pl.ds(0, 31 * count)], left)
    Wires(send_v, recv_v).drain(vals.at[pl.ds(0, 48)], left)


def fused(blk, pao_size, cabs_size, pao, cabs, weight):
    dma = pltpu.SemaphoreType.DMA
    vmem = pl.BlockSpec(memory_space=pltpu.VMEM)
    hbm = pl.BlockSpec(memory_space=pltpu.HBM)
    f32 = jnp.float32
    return pl.pallas_call(
        kernel,
        out_shape=jax.ShapeDtypeStruct((64, 24, 96), f32),
        in_specs=[hbm] * 6,
        out_specs=vmem,
        scratch_shapes=[
            pltpu.SMEM((4, 64), jnp.int32),
            pltpu.SMEM((64,), jnp.int32),
            pltpu.SMEM((64,), jnp.int32),
            pltpu.VMEM((4, 64), jnp.int32),
            pltpu.VMEM((2, 48), jnp.bfloat16),
            pltpu.VMEM((144, 3840), jnp.bfloat16),
            pltpu.VMEM((64, 48, 1920), jnp.bfloat16),
            pltpu.VMEM((2, 768, 1920), jnp.bfloat16),
            pltpu.VMEM((CHOSEN, 8, 128), f32),
            [pltpu.VMEM((4, n, 8, 128), f32) for _, _, n in PARTS],
            [pltpu.VMEM((2, (n + 1) // 2, 8, 128), f32) for _, _, n in PARTS],
            [pltpu.VMEM((2, n, 8, 128), f32) for _, _, n in PARTS],
            pltpu.VMEM((32 * HELD, 8, 128), f32),
            pltpu.VMEM((64, 24, 384), f32),
            pltpu.VMEM((16, 24, 384), f32),
            pltpu.VMEM((32, 24, 384), f32),
            dma,
            dma((Gather.TOTAL + 4,)),
            dma((len(PARTS),)),
            dma((3 * len(PARTS),)),
            dma((len(PARTS),)),
            dma((31 * len(PARTS),)),
            dma,
            dma((24,)),
            dma((9,)),
        ],
        compiler_params=pltpu.CompilerParams(
            collective_id=0, has_side_effects=True, vmem_limit_bytes=56 * 1024 * 1024
        ),
        name="fused",
    )(blk, pao_size, cabs_size, pao, cabs, weight)


def shards(pao_blocks, cabs_blocks, cabs_weight, pair_blocks, pao_size, cabs_size):
    return fused(
        pair_blocks.T,
        pao_size,
        cabs_size,
        pao_blocks.reshape(48, -1),
        cabs_blocks.reshape(96, -1),
        cabs_weight,
    )


def solution(mesh):
    placed = (
        P("atom", None, "aux"),
        P("atom", None, "aux"),
        P("atom", None),
        P("atom", None),
        P("atom"),
        P("atom"),
    )
    return jax.shard_map(
        shards, mesh=mesh, in_specs=placed, out_specs=P("atom", "aux", None), check_vma=False
    )
```
